8 devices in a mesh: dp: 1 (over z), hp: 2 (over y), sp: 4 (over x, core).
Axes of the slice: x: 2, y: 2, z: 1, core: 2. Of those that a mesh axis runs over, the one named last changes fastest.
Arguments:
- x_in: bfloat16 [4096, 4096], P(('dp', 'sp', 'hp'))
- w_q: bfloat16 [4096, 4096], P(None, 'hp')
- w_k: bfloat16 [4096, 4096], P(None, 'hp')
- w_v: bfloat16 [4096, 4096], P(None, 'hp')
- w_o: bfloat16 [4096, 4096], P('hp')
Outputs:
- output: bfloat16 [4096, 4096], P(('dp', 'sp', 'hp'))
All inputs are finite; a program needn't handle non-finite values.
Results may differ from the reference program's by a relative error of at most 0.00691038.
Values are sent between devices in bfloat16 or wider.
A program may use at most 1 GiB of HBM per device.

```python
import math
import jax
import jax.numpy as jnp
from jax import lax

D = 4096
H = 32
HKV = 32
HEAD = 128
SEQ = 4096
QBLK = 64
GROUP = H // HKV


def setup_inputs(seed: int = 0, part: int = 0) -> dict:
    root = jax.random.key(seed)
    shared_key, part_root = jax.random.split(root)
    part_key = jax.random.fold_in(part_root, part)
    key_q, key_k, key_v, key_o = jax.random.split(shared_key, 4)
    logit_std = math.sqrt(max(math.log(SEQ / 16.0), 1.0))
    qk_gain = math.sqrt(logit_std) / math.sqrt(D)
    x_in = jax.random.normal(part_key, (SEQ, D), jnp.float32).astype(jnp.bfloat16)
    w_q = (jax.random.normal(key_q, (D, H * HEAD), jnp.float32) * qk_gain).astype(jnp.bfloat16)
    w_k = (jax.random.normal(key_k, (D, HKV * HEAD), jnp.float32) * qk_gain).astype(jnp.bfloat16)
    w_v = (jax.random.normal(key_v, (D, HKV * HEAD), jnp.float32) / math.sqrt(D)).astype(jnp.bfloat16)
    w_o = (jax.random.normal(key_o, (H * HEAD, D), jnp.float32) * (4.0 / math.sqrt(H * HEAD))).astype(jnp.bfloat16)
    return {'x_in': x_in, 'w_q': w_q, 'w_k': w_k, 'w_v': w_v, 'w_o': w_o}


def reference(x_in, w_q, w_k, w_v, w_o):
    q_all = jnp.dot(x_in, w_q, preferred_element_type=jnp.float32).astype(jnp.bfloat16)
    k_all = jnp.dot(x_in, w_k, preferred_element_type=jnp.float32).astype(jnp.bfloat16)
    v_all = jnp.dot(x_in, w_v, preferred_element_type=jnp.float32).astype(jnp.bfloat16)
    q_heads = q_all.astype(jnp.float32).reshape(SEQ, HKV, GROUP, HEAD)
    k_heads = k_all.astype(jnp.float32).reshape(SEQ, HKV, HEAD)
    v_heads = v_all.astype(jnp.float32).reshape(SEQ, HKV, HEAD)
    attn_scale = 1.0 / math.sqrt(HEAD)

    def query_block(blk_index):
        q_blk = lax.dynamic_slice_in_dim(q_heads, blk_index * QBLK, QBLK, 0)
        scores = jnp.einsum('qhgd,khd->hgqk', q_blk, k_heads) * attn_scale
        row_max = jnp.max(scores, axis=-1, keepdims=True)
        prob_vals = jnp.exp(scores - row_max)
        row_sum = jnp.sum(prob_vals, axis=-1, keepdims=True)
        weighted = jnp.einsum('hgqk,khd->hgqd', prob_vals.astype(jnp.bfloat16).astype(jnp.float32), v_heads)
        out_blk = (weighted / row_sum).astype(jnp.bfloat16)
        return jnp.transpose(out_blk, (2, 0, 1, 3)).reshape(QBLK, H * HEAD)

    o_all = lax.map(query_block, jnp.arange(SEQ // QBLK)).reshape(SEQ, H * HEAD)
    return jnp.dot(o_all, w_o, preferred_element_type=jnp.float32).astype(jnp.bfloat16)
```

```python
import functools
import math

import jax
import jax.numpy as jnp
from jax import lax
from jax.experimental import pallas as pl
from jax.experimental.pallas import tpu as pltpu
from jax.sharding import PartitionSpec as P


HEAD_DIM = 128
EXP2_SCALE = math.log2(math.e) / math.sqrt(HEAD_DIM)


def attend_kernel(groups, first, last, *refs):
    q_ref, k_refs, v_refs = refs[0], refs[1:1 + groups], refs[1 + groups:1 + 2 * groups]
    pos = 1 + 2 * groups
    if not first:
        m_in, l_in, acc_in = refs[pos:pos + 3]
        pos += 3
    outs = refs[pos:]
    q = q_ref[...]

    def scores_of(g):
        return lax.dot_general(k_refs[g][...], q, (((1,), (1,)), ((), ())), preferred_element_type=jnp.float32)

    if not first:
        run_max, run_sum, acc = m_in[0], l_in[0], acc_in[...]
    scores = scores_of(0)
    for g in range(groups):
        following = scores_of(g + 1) if g + 1 < groups else None
        scaled = scores * EXP2_SCALE
        new_max = jnp.max(scaled, axis=0, keepdims=True)
        if first and g == 0:
            probs = jnp.exp2(scaled - new_max)
            run_sum = jnp.sum(probs, axis=0, keepdims=True)
            acc = jnp.dot(v_refs[g][...], probs.astype(jnp.bfloat16), preferred_element_type=jnp.float32)
        else:
            new_max = jnp.maximum(run_max, new_max)
            fade = jnp.exp2(run_max - new_max)
            probs = jnp.exp2(scaled - new_max)
            run_sum = run_sum * fade + jnp.sum(probs, axis=0, keepdims=True)
            acc = acc * fade + jnp.dot(v_refs[g][...], probs.astype(jnp.bfloat16), preferred_element_type=jnp.float32)
        run_max, scores = new_max, following
    if last:
        outs[0][...] = (acc / run_sum).T.astype(jnp.bfloat16)
    else:
        outs[0][0], outs[1][0], outs[2][...] = run_max, run_sum, acc


def attend(q, keys, values_t, state, last):
    groups, rows, heads = len(keys), q.shape[0], q.shape[1] // HEAD_DIM
    first = state is None
    state_specs = [
        pl.BlockSpec((1, 1, rows), lambda h: (h, 0, 0)),
        pl.BlockSpec((1, 1, rows), lambda h: (h, 0, 0)),
        pl.BlockSpec((HEAD_DIM, rows), lambda h: (h, 0)),
    ]
    state_shapes = [jax.ShapeDtypeStruct((heads, 1, rows), jnp.float32)] * 2
    state_shapes.append(jax.ShapeDtypeStruct((heads * HEAD_DIM, rows), jnp.float32))
    q_spec = pl.BlockSpec((rows, HEAD_DIM), lambda h: (0, h))
    in_specs = [q_spec]
    in_specs += [pl.BlockSpec((k.shape[0], HEAD_DIM), lambda h: (0, h)) for k in keys]
    in_specs += [pl.BlockSpec((HEAD_DIM, v.shape[1]), lambda h: (h, 0)) for v in values_t]
    in_specs += [] if first else state_specs
    key_rows = sum(k.shape[0] for k in keys)
    return pl.pallas_call(
        functools.partial(attend_kernel, groups, first, last),
        grid=(heads,),
        in_specs=in_specs,
        out_specs=q_spec if last else state_specs,
        out_shape=jax.ShapeDtypeStruct(q.shape, jnp.bfloat16) if last else state_shapes,
        input_output_aliases={} if first or last else {1 + 2 * groups + j: j for j in range(3)},
        cost_estimate=pl.CostEstimate(
            flops=8 * rows * key_rows * heads * HEAD_DIM,
            bytes_accessed=2 * heads * HEAD_DIM * (rows + 2 * key_rows),
            transcendentals=rows * key_rows * heads,
        ),
        compiler_params=pltpu.CompilerParams(vmem_limit_bytes=48 * 2**20),
    )(q, *keys, *values_t, *(state or ()))


def project(x, w):
    return jnp.dot(x, w, preferred_element_type=jnp.float32).astype(jnp.bfloat16)


def project_t(x, w):
    return lax.dot_general(w, x, (((0,), (1,)), ((), ())), preferred_element_type=jnp.float32).astype(jnp.bfloat16)


def solution(mesh):
    hp_swap = [(0, 1), (1, 0)]
    x_swap = [(0, 2), (1, 3), (2, 0), (3, 1)]
    core_swap = [(0, 1), (1, 0), (2, 3), (3, 2)]

    def device_fn(x_own, w_q, w_k, w_v, w_o):
        sp = lax.axis_index('sp')
        quarter = w_o.shape[0] // 4
        over_y = lambda a: lax.ppermute(a, 'hp', hp_swap)
        over_x = lambda a: lax.ppermute(a, 'sp', x_swap)
        over_core = lambda a: lax.ppermute(a, 'sp', core_swap)

        x_far = over_y(x_own)
        wo_y = over_y(lax.dynamic_slice_in_dim(w_o, sp * quarter, quarter, 0))

        k_o = project(x_own, w_k)
        v_o = project_t(x_own, w_v)
        q_o = project(x_own, w_q)
        k_xo, v_xo = over_x(k_o), over_x(v_o)
        k_so, v_so = over_core(k_o), over_core(v_o)
        k_r = project(x_far, w_k)
        v_r = project_t(x_far, w_v)
        q_r = project(x_far, w_q)
        k_xr, v_xr = over_x(k_r), over_x(v_r)
        k_sr, v_sr = over_core(k_r), over_core(v_r)
        k_sxo, v_sxo = over_core(k_xo), over_core(v_xo)
        wo_x = over_x(wo_y)
        k_sxr, v_sxr = over_core(k_xr), over_core(v_xr)
        wo_sy = over_core(wo_y)
        wo_sx = over_core(wo_x)

        early_k = [k_o, k_so, k_r, k_sr, k_xo, k_sxo]
        early_v = [v_o, v_so, v_r, v_sr, v_xo, v_sxo]
        late_k, late_v = [k_xr, k_sxr], [v_xr, v_sxr]
        state_r = attend(q_r, early_k, early_v, None, False)
        state_o = attend(q_o, early_k, early_v, None, False)
        o_r = attend(q_r, late_k, late_v, state_r, True)
        o_far = over_y(o_r)
        o_own = attend(q_o, late_k, late_v, state_o, True)
        total = jnp.dot(o_own, w_o, preferred_element_type=jnp.float32)
        for rank, piece in ((sp, wo_y), (sp ^ 2, wo_x), (sp ^ 1, wo_sy), (sp ^ 3, wo_sx)):
            part = lax.dynamic_slice_in_dim(o_far, rank * quarter, quarter, 1)
            total += jnp.dot(part, piece, preferred_element_type=jnp.float32)
        return total.astype(jnp.bfloat16)

    seq_spec = P(('dp', 'sp', 'hp'), None)
    in_specs = (seq_spec, P(None, 'hp'), P(None, 'hp'), P(None, 'hp'), P('hp', None))
    return jax.shard_map(device_fn, mesh=mesh, in_specs=in_specs, out_specs=seq_spec, check_vma=False)
```

```python
import functools
import math

import jax
import jax.numpy as jnp
from jax import lax
from jax.experimental import pallas as pl
from jax.experimental.pallas import tpu as pltpu
from jax.sharding import PartitionSpec as P


HEAD_DIM = 128
EXP2_SCALE = math.log2(math.e) / math.sqrt(HEAD_DIM)


def attend_kernel(groups, first, last, *refs):
    q_ref, k_refs, v_refs = refs[0], refs[1:1 + groups], refs[1 + groups:1 + 2 * groups]
    pos = 1 + 2 * groups
    if not first:
        m_in, l_in, acc_in = refs[pos:pos + 3]
        pos += 3
    outs = refs[pos:]
    q = q_ref[...]

    def scores_of(g):
        return lax.dot_general(k_refs[g][...], q, (((1,), (1,)), ((), ())), preferred_element_type=jnp.float32)

    if not first:
        run_max, run_sum, acc = m_in[0], l_in[0], acc_in[...]
    ahead = [scores_of(g) for g in range(min(2, groups))]
    for g in range(groups):
        if g + 2 < groups:
            ahead.append(scores_of(g + 2))
        scores = ahead.pop(0)
        new_max = jnp.max(scores, axis=0, keepdims=True) * EXP2_SCALE
        fade = None
        if not (first and g == 0):
            new_max = jnp.maximum(run_max, new_max)
            fade = jnp.exp2(run_max - new_max)
        probs = jnp.exp2(scores * EXP2_SCALE - new_max)
        part_sum = jnp.sum(probs, axis=0, keepdims=True)
        part = jnp.dot(v_refs[g][...], probs.astype(jnp.bfloat16), preferred_element_type=jnp.float32)
        if fade is None:
            run_sum, acc = part_sum, part
        else:
            run_sum, acc = run_sum * fade + part_sum, acc * fade + part
        run_max = new_max
    if last:
        outs[0][...] = (acc / run_sum).T.astype(jnp.bfloat16)
    else:
        outs[0][0], outs[1][0], outs[2][...] = run_max, run_sum, acc


def attend(q, keys, values_t, state, last):
    groups, rows, heads = len(keys), q.shape[0], q.shape[1] // HEAD_DIM
    first = state is None
    state_specs = [
        pl.BlockSpec((1, 1, rows), lambda h: (h, 0, 0)),
        pl.BlockSpec((1, 1, rows), lambda h: (h, 0, 0)),
        pl.BlockSpec((HEAD_DIM, rows), lambda h: (h, 0)),
    ]
    state_shapes = [jax.ShapeDtypeStruct((heads, 1, rows), jnp.float32)] * 2
    state_shapes.append(jax.ShapeDtypeStruct((heads * HEAD_DIM, rows), jnp.float32))
    q_spec = pl.BlockSpec((rows, HEAD_DIM), lambda h: (0, h))
    in_specs = [q_spec]
    in_specs += [pl.BlockSpec((k.shape[0], HEAD_DIM), lambda h: (0, h)) for k in keys]
    in_specs += [pl.BlockSpec((HEAD_DIM, v.shape[1]), lambda h: (h, 0)) for v in values_t]
    in_specs += [] if first else state_specs
    key_rows = sum(k.shape[0] for k in keys)
    return pl.pallas_call(
        functools.partial(attend_kernel, groups, first, last),
        grid=(heads,),
        in_specs=in_specs,
        out_specs=q_spec if last else state_specs,
        out_shape=jax.ShapeDtypeStruct(q.shape, jnp.bfloat16) if last else state_shapes,
        input_output_aliases={} if first or last else {1 + 2 * groups + j: j for j in range(3)},
        cost_estimate=pl.CostEstimate(
            flops=8 * rows * key_rows * heads * HEAD_DIM,
            bytes_accessed=2 * heads * HEAD_DIM * (rows + 2 * key_rows),
            transcendentals=rows * key_rows * heads,
        ),
        compiler_params=pltpu.CompilerParams(vmem_limit_bytes=48 * 2**20),
    )(q, *keys, *values_t, *(state or ()))


def project(x, w):
    return jnp.dot(x, w, preferred_element_type=jnp.float32).astype(jnp.bfloat16)


def project_t(x, w):
    return lax.dot_general(w, x, (((0,), (1,)), ((), ())), preferred_element_type=jnp.float32).astype(jnp.bfloat16)


def fold_kernel(pairs, has_base, ranks_ref, *refs):
    total = refs[2 * pairs][...] if has_base else None
    for i in range(pairs):
        part = jnp.dot(refs[i][...], refs[pairs + i][...], preferred_element_type=jnp.float32)
        total = part if total is None else total + part
    refs[-1][...] = total.astype(refs[-1].dtype)


def fold(lhs, pieces, ranks, base, dtype, width=512):
    rows, columns, count = lhs.shape[0], pieces[0].shape[1], len(pieces)
    depth = pieces[0].shape[0]
    lhs_specs = [pl.BlockSpec((rows, depth), functools.partial(lambda i, j, r: (0, r[i]), i)) for i in range(count)]
    rhs_specs = [pl.BlockSpec((depth, width), lambda j, r: (0, j)) for _ in pieces]
    out_spec = pl.BlockSpec((rows, width), lambda j, r: (0, j))
    return pl.pallas_call(
        functools.partial(fold_kernel, count, base is not None),
        grid_spec=pltpu.PrefetchScalarGridSpec(
            num_scalar_prefetch=1,
            grid=(columns // width,),
            in_specs=lhs_specs + rhs_specs + ([out_spec] if base is not None else []),
            out_specs=out_spec,
        ),
        out_shape=jax.ShapeDtypeStruct((rows, columns), dtype),
        cost_estimate=pl.CostEstimate(
            flops=2 * rows * columns * depth * count,
            bytes_accessed=2 * columns * depth * count,
            transcendentals=0,
        ),
        compiler_params=pltpu.CompilerParams(vmem_limit_bytes=48 * 2**20),
    )(jnp.stack(ranks).astype(jnp.int32), *([lhs] * count), *pieces, *(() if base is None else (base,)))


def after(value, *tokens):
    return lax.optimization_barrier((value, *tokens))[0]


def solution(mesh):
    hp_swap = [(0, 1), (1, 0)]
    x_swap = [(0, 2), (1, 3), (2, 0), (3, 1)]
    core_swap = [(0, 1), (1, 0), (2, 3), (3, 2)]

    def device_fn(x_own, w_q, w_k, w_v, w_o):
        sp = lax.axis_index('sp')
        quarter = w_o.shape[0] // 4
        over_y = lambda a: lax.ppermute(a, 'hp', hp_swap)
        over_x = lambda a: lax.ppermute(a, 'sp', x_swap)
        over_core = lambda a: lax.ppermute(a, 'sp', core_swap)

        x_far = over_y(x_own)
        k_o = project(x_own, w_k)
        k_xo, k_so = over_x(k_o), over_core(k_o)
        v_o = project_t(after(x_own, k_o), w_v)
        v_xo, v_so = over_x(v_o), over_core(v_o)
        wo_part = lax.dynamic_slice_in_dim(after(w_o, v_o), sp * quarter, quarter, 0)
        wo_y = over_y(wo_part)
        q_o = project(after(x_own, wo_part), w_q)
        state_o = attend(after(q_o, v_o), [k_o, k_so], [v_o, v_so], None, False)

        x_far = after(x_far, state_o[0])
        k_r = project(x_far, w_k)
        k_xr, k_sr = over_x(k_r), over_core(k_r)
        v_r = project_t(after(x_far, k_r), w_v)
        v_xr, v_sr = over_x(v_r), over_core(v_r)
        k_sxo, v_sxo = over_core(after(k_xo, v_r)), over_core(after(v_xo, v_r))
        q_r = project(after(x_far, v_r), w_q)
        state_r = attend(q_r, [k_o, k_so, k_r, k_sr, k_xo, k_sxo], [v_o, v_so, v_r, v_sr, v_xo, v_sxo], None, False)
        wo_sy = over_core(after(wo_y, state_r[0]))
        state_o = attend(after(q_o, state_r[0]), [k_r, k_sr, k_xo, k_sxo], [v_r, v_sr, v_xo, v_sxo], state_o, False)

        k_sxr, v_sxr = over_core(after(k_xr, state_o[0])), over_core(after(v_xr, state_o[0]))
        wo_x = over_x(after(wo_y, state_o[0]))
        late_k, late_v = [k_xr, k_sxr], [v_xr, v_sxr]
        o_r = attend(q_r, late_k, late_v, state_r, True)
        o_far = over_y(o_r)
        o_own = attend(after(q_o, o_r), late_k, late_v, state_o, True)
        total = fold(o_own, [w_o], [sp * 0], None, jnp.float32)
        o_far = after(o_far, total)
        total = fold(o_far, [wo_y, wo_sy], [sp, sp ^ 1], total, jnp.float32)
        wo_x = after(wo_x, total)
        wo_sx = over_core(wo_x)
        return fold(o_far, [wo_x, wo_sx], [sp ^ 2, sp ^ 3], total, jnp.bfloat16)

    seq_spec = P(('dp', 'sp', 'hp'), None)
    in_specs = (seq_spec, P(None, 'hp'), P(None, 'hp'), P(None, 'hp'), P('hp', None))
    return jax.shard_map(device_fn, mesh=mesh, in_specs=in_specs, out_specs=seq_spec, check_vma=False)
```

```python
import functools
import math

import jax
import jax.numpy as jnp
from jax import lax
from jax.experimental import pallas as pl
from jax.experimental.pallas import tpu as pltpu
from jax.sharding import PartitionSpec as P


HEAD_DIM = 128
EXP2_SCALE = math.log2(math.e) / math.sqrt(HEAD_DIM)


def attend_kernel(shape, heads, first, last, *refs):
    refs = list(refs)
    take = lambda n: [refs.pop(0) for _ in range(n)]
    q_refs = take(shape[0])
    groups = [(take(k), take(v)) for k, v in shape[1:]]
    state_in = None if first else take(3)
    outs = refs
    at = lambda h: slice(h * HEAD_DIM, (h + 1) * HEAD_DIM)
    queries = [jnp.concatenate([r[:, at(h)] for r in q_refs], axis=0) for h in range(heads)]

    def scores_of(h, g):
        parts = [
            lax.dot_general(k[:, at(h)], queries[h], (((1,), (1,)), ((), ())), preferred_element_type=jnp.float32)
            for k in groups[g][0]
        ]
        return parts[0] if len(parts) == 1 else jnp.concatenate(parts, axis=0)

    items = [(h, g) for g in range(len(groups)) for h in range(heads)]
    depth = 2
    state = {} if first else {h: (state_in[0][h], state_in[1][h], state_in[2][at(h), :]) for h in range(heads)}
    ahead = [scores_of(*items[i]) for i in range(min(depth, len(items)))]
    for i, (h, g) in enumerate(items):
        if i + depth < len(items):
            ahead.append(scores_of(*items[i + depth]))
        scores = ahead.pop(0)
        new_max = jnp.max(scores, axis=0, keepdims=True) * EXP2_SCALE
        if h in state:
            new_max = jnp.maximum(state[h][0], new_max)
        probs = jnp.exp2(scores * EXP2_SCALE - new_max)
        part_sum = jnp.sum(probs, axis=0, keepdims=True)
        probs = probs.astype(jnp.bfloat16)
        part, row = None, 0
        for v in groups[g][1]:
            count = v.shape[1]
            piece = jnp.dot(v[at(h), :], probs[row:row + count], preferred_element_type=jnp.float32)
            part = piece if part is None else part + piece
            row += count
        if h in state:
            run_max, run_sum, acc = state[h]
            fade = jnp.exp2(run_max - new_max)
            state[h] = (new_max, run_sum * fade + part_sum, acc * fade + part)
        else:
            state[h] = (new_max, part_sum, part)
    for h in range(heads):
        run_max, run_sum, acc = state[h]
        if last:
            outs[0][:, at(h)] = (acc / run_sum).T.astype(jnp.bfloat16)
        else:
            outs[0][h], outs[1][h], outs[2][at(h), :] = run_max, run_sum, acc


def attend(queries, groups, state, last, block=1):
    rows, heads = sum(q.shape[0] for q in queries), queries[0].shape[1] // HEAD_DIM
    width = block * HEAD_DIM
    first = state is None
    state_specs = [
        pl.BlockSpec((block, 1, rows), lambda h: (h, 0, 0)),
        pl.BlockSpec((block, 1, rows), lambda h: (h, 0, 0)),
        pl.BlockSpec((width, rows), lambda h: (h, 0)),
    ]
    state_shapes = [jax.ShapeDtypeStruct((heads, 1, rows), jnp.float32)] * 2
    state_shapes.append(jax.ShapeDtypeStruct((heads * HEAD_DIM, rows), jnp.float32))
    tall = lambda a: pl.BlockSpec((a.shape[0], width), lambda h: (0, h))
    wide = lambda a: pl.BlockSpec((width, a.shape[1]), lambda h: (h, 0))
    operands, in_specs, shape, key_rows = list(queries), [tall(q) for q in queries], [len(queries)], 0
    for keys, values_t in groups:
        operands += [*keys, *values_t]
        in_specs += [tall(k) for k in keys] + [wide(v) for v in values_t]
        shape.append((len(keys), len(values_t)))
        key_rows += sum(k.shape[0] for k in keys)
    count = len(operands)
    o_shape = jax.ShapeDtypeStruct((rows, heads * HEAD_DIM), jnp.bfloat16)
    return pl.pallas_call(
        functools.partial(attend_kernel, tuple(shape), block, first, last),
        grid=(heads // block,),
        in_specs=in_specs + ([] if first else state_specs),
        out_specs=pl.BlockSpec((rows, width), lambda h: (0, h)) if last else state_specs,
        out_shape=o_shape if last else state_shapes,
        input_output_aliases={} if first or last else {count + j: j for j in range(3)},
        cost_estimate=pl.CostEstimate(
            flops=8 * rows * key_rows * heads * HEAD_DIM,
            bytes_accessed=2 * heads * HEAD_DIM * (rows + 2 * key_rows),
            transcendentals=rows * key_rows * heads,
        ),
        compiler_params=pltpu.CompilerParams(vmem_limit_bytes=48 * 2**20),
    )(*operands, *(state or ()))


def project_kernel(flips, width, x_ref, *refs):
    count = len(flips)
    w_refs, o_refs, (ring, sems) = refs[:count], refs[count:2 * count], refs[2 * count:]
    steps = [w.shape[1] // width for w in w_refs]
    firsts = [sum(steps[:i]) for i in range(count)]

    def copy(i, step, slot):
        columns = pl.ds(pl.multiple_of(step * width, width), width)
        return pltpu.make_async_copy(w_refs[i].at[:, columns], ring.at[slot], sems.at[slot])

    def fetch(n):
        for i in range(count):
            @pl.when(jnp.logical_and(n >= firsts[i], n < firsts[i] + steps[i]))
            def _():
                copy(i, n - firsts[i], lax.rem(n, 3)).start()

    fetch(jnp.int32(0))
    fetch(jnp.int32(1))
    for i in range(count):
        def step(j, carry, i=i):
            n = firsts[i] + j
            slot = lax.rem(n, 3)
            fetch(n + 2)
            copy(i, j, slot).wait()
            block = jnp.dot(x_ref[...], ring[slot], preferred_element_type=jnp.float32)
            columns = pl.ds(pl.multiple_of(j * width, width), width)
            if flips[i]:
                o_refs[i][columns, :] = block.T.astype(jnp.bfloat16)
            else:
                o_refs[i][:, columns] = block.astype(jnp.bfloat16)
            return carry

        lax.fori_loop(0, steps[i], step, 0)


def project(x, weights, flips, width=512):
    rows, depth = x.shape
    shapes = [(w.shape[1], rows) if f else (rows, w.shape[1]) for w, f in zip(weights, flips)]
    return pl.pallas_call(
        functools.partial(project_kernel, tuple(flips), width),
        in_specs=[pl.BlockSpec(memory_space=pltpu.VMEM)] + [pl.BlockSpec(memory_space=pl.ANY)] * len(weights),
        out_specs=[pl.BlockSpec(memory_space=pltpu.VMEM)] * len(weights),
        out_shape=[jax.ShapeDtypeStruct(s, jnp.bfloat16) for s in shapes],
        scratch_shapes=[pltpu.VMEM((3, depth, width), jnp.bfloat16), pltpu.SemaphoreType.DMA((3,))],
        cost_estimate=pl.CostEstimate(
            flops=2 * rows * depth * sum(w.shape[1] for w in weights),
            bytes_accessed=2 * depth * sum(w.shape[1] for w in weights),
            transcendentals=0,
        ),
        compiler_params=pltpu.CompilerParams(vmem_limit_bytes=40 * 2**20),
    )(x, *weights)


def fold_kernel(depths, has_base, first_unit, lhs_ref, *refs):
    total = refs[len(depths)][...] if has_base else None
    for i, depth in enumerate(depths):
        start = pl.multiple_of(first_unit[i] * 128, 128)
        part = jnp.dot(lhs_ref[:, pl.ds(start, depth)], refs[i][...], preferred_element_type=jnp.float32)
        total = part if total is None else total + part
    refs[-1][...] = total.astype(refs[-1].dtype)


def fold(lhs, pieces, units, base, dtype, width=512):
    rows, columns = lhs.shape[0], pieces[0].shape[1]
    depths = tuple(p.shape[0] for p in pieces)
    out_spec = pl.BlockSpec((rows, width), lambda j, r: (0, j))
    return pl.pallas_call(
        functools.partial(fold_kernel, depths, base is not None),
        grid_spec=pltpu.PrefetchScalarGridSpec(
            num_scalar_prefetch=1,
            grid=(columns // width,),
            in_specs=[pl.BlockSpec(lhs.shape, lambda j, r: (0, 0))]
            + [pl.BlockSpec((d, width), lambda j, r: (0, j)) for d in depths]
            + ([out_spec] if base is not None else []),
            out_specs=out_spec,
        ),
        out_shape=jax.ShapeDtypeStruct((rows, columns), dtype),
        cost_estimate=pl.CostEstimate(
            flops=2 * rows * columns * sum(depths),
            bytes_accessed=2 * columns * sum(depths),
            transcendentals=0,
        ),
        compiler_params=pltpu.CompilerParams(vmem_limit_bytes=48 * 2**20),
    )(jnp.stack(units).astype(jnp.int32), lhs, *pieces, *(() if base is None else (base,)))


def after(value, *tokens):
    return lax.optimization_barrier((value, *tokens))[0]


def solution(mesh):
    hp_swap = [(0, 1), (1, 0)]
    x_swap = [(0, 2), (1, 3), (2, 0), (3, 1)]
    core_swap = [(0, 1), (1, 0), (2, 3), (3, 2)]

    def device_fn(x_own, w_q, w_k, w_v, w_o):
        sp = lax.axis_index('sp')
        chip, core = sp // 2, sp % 2
        half = x_own.shape[0] // 2
        over_y = lambda a: lax.ppermute(a, 'hp', hp_swap)
        over_x = lambda a: lax.ppermute(a, 'sp', x_swap)
        over_core = lambda a: lax.ppermute(a, 'sp', core_swap)

        unit_a = lambda chip_, core_: chip_ * 10 + core_ * 3
        unit_b = lambda core_: 6 + core_ * 2

        x_f0 = over_y(x_own[:half])
        (k_o,) = project(x_own, [w_k], [False])
        k_xo = over_x(k_o)
        x_f1 = over_y(after(x_own, k_o)[half:])
        v_o, q_o = project(after(x_own, k_o), [w_v, w_q], [True, False])
        v_xo = over_x(v_o)
        rows_a = lax.dynamic_slice_in_dim(after(w_o, v_o), unit_a(chip, core) * 128, 384, 0)
        rows_b = lax.dynamic_slice_in_dim(after(w_o, v_o), unit_b(core) * 128, 256, 0)
        wa = over_y(rows_a)
        wb = over_y(after(rows_b, rows_a))
        k_so, v_so = over_core(after(k_o, v_o)), over_core(v_o)

        all_w, all_f = [w_k, w_v, w_q], [False, True, False]
        k_r0, v_r0, q_r0 = project(after(x_f0, rows_a, rows_b), all_w, all_f)
        k_xr0, v_xr0 = over_x(k_r0), over_x(v_r0)
        k_sr0, v_sr0 = over_core(k_r0), over_core(v_r0)
        own, own_s = ([k_o], [v_o]), ([k_so], [v_so])
        state_o = attend([after(q_o, q_r0)], [own, own_s], None, False, 4)

        k_r1, v_r1, q_r1 = project(after(x_f1, state_o[0]), all_w, all_f)
        k_xr1, v_xr1 = over_x(k_r1), over_x(v_r1)
        k_sr1, v_sr1 = over_core(k_r1), over_core(v_r1)
        k_sxo, v_sxo = over_core(after(k_xo, q_r0)), over_core(after(v_xo, v_r1))
        far, far_s = ([k_r0, k_r1], [v_r0, v_r1]), ([k_sr0, k_sr1], [v_sr0, v_sr1])
        xo, xo_s = ([k_xo], [v_xo]), ([k_sxo], [v_sxo])
        state_r = attend([q_r0, q_r1], [own, own_s, far, far_s, xo, xo_s], None, False, 2)
        k_sxr0, v_sxr0 = over_core(after(k_xr0, state_r[0])), over_core(after(v_xr0, state_r[0]))
        state_o = attend([after(q_o, state_r[0])], [far, far_s, xo, xo_s], state_o, False, 2)
        wx = over_x(after(wa, state_o[0]))
        wa_s = over_core(after(wa, state_o[0]))
        late = ([k_xr0, k_sxr0], [v_xr0, v_sxr0])
        state_r = attend([after(q_r0, state_o[0]), q_r1], [late], state_r, False, 8)
        state_o = attend([after(q_o, state_r[0])], [late], state_o, False, 8)

        k_sxr1, v_sxr1 = over_core(after(k_xr1, state_o[0])), over_core(after(v_xr1, state_o[0]))
        latest = ([k_xr1, k_sxr1], [v_xr1, v_sxr1])
        o_r = attend([q_r0, q_r1], [latest], state_r, True, 8)
        o_f = over_y(o_r)
        o_own = attend([after(q_o, o_r)], [latest], state_o, True, 8)
        wb_s = over_core(after(wb, o_own))
        total = fold(o_own, [w_o], [sp * 0], None, jnp.float32)
        o_f = after(o_f, total)
        total = fold(
            o_f,
            [wa, wa_s, wb, wb_s],
            [unit_a(chip, core), unit_a(chip, 1 - core), unit_b(core), unit_b(1 - core)],
            total,
            jnp.float32,
        )
        wx = after(wx, total)
        wx_s = over_core(wx)
        return fold(o_f, [wx, wx_s], [unit_a(1 - chip, core), unit_a(1 - chip, 1 - core)], total, jnp.bfloat16)

    seq_spec = P(('dp', 'sp', 'hp'), None)
    in_specs = (seq_spec, P(None, 'hp'), P(None, 'hp'), P(None, 'hp'), P('hp', None))
    return jax.shard_map(device_fn, mesh=mesh, in_specs=in_specs, out_specs=seq_spec, check_vma=False)
```

```python
import functools
import math

import jax
import jax.numpy as jnp
from jax import lax
from jax.experimental import pallas as pl
from jax.experimental.pallas import tpu as pltpu
from jax.sharding import PartitionSpec as P


HEAD_DIM = 128
EXP2_SCALE = math.log2(math.e) / math.sqrt(HEAD_DIM)


def attend_kernel(shape, heads, half, first, last, *refs):
    refs = list(refs)
    take = lambda n: [refs.pop(0) for _ in range(n)]
    q_refs = take(shape[0])
    groups = [([take(k) for k in widths], take(v)) for widths, v in shape[1:]]
    state_in = None if first else take(3)
    outs = refs
    at = lambda h: slice(h * HEAD_DIM, (h + 1) * HEAD_DIM)
    queries = [jnp.concatenate([r[:, at(h)] for r in q_refs], axis=0) for h in range(heads)]
    low = pl.program_id(0) < half

    def keys_of(piece, h):
        if len(piece) == 1:
            return piece[0][:, at(h)]
        return jnp.where(low, piece[0][:, at(h)], piece[1][:, at(h)])

    def scores_of(h, g):
        parts = [
            lax.dot_general(keys_of(k, h), queries[h], (((1,), (1,)), ((), ())), preferred_element_type=jnp.float32)
            for k in groups[g][0]
        ]
        return parts[0] if len(parts) == 1 else jnp.concatenate(parts, axis=0)

    items = [(h, g) for g in range(len(groups)) for h in range(heads)]
    depth = 2
    state = {} if first else {h: (state_in[0][h], state_in[1][h], state_in[2][at(h), :]) for h in range(heads)}
    ahead = [scores_of(*items[i]) for i in range(min(depth, len(items)))]
    for i, (h, g) in enumerate(items):
        if i + depth < len(items):
            ahead.append(scores_of(*items[i + depth]))
        scores = ahead.pop(0)
        new_max = jnp.max(scores, axis=0, keepdims=True) * EXP2_SCALE
        if h in state:
            new_max = jnp.maximum(state[h][0], new_max)
        probs = jnp.exp2(scores * EXP2_SCALE - new_max)
        part_sum = jnp.sum(probs, axis=0, keepdims=True)
        probs = probs.astype(jnp.bfloat16)
        part, row = None, 0
        for v in groups[g][1]:
            count = v.shape[1]
            piece = jnp.dot(v[at(h), :], probs[row:row + count], preferred_element_type=jnp.float32)
            part = piece if part is None else part + piece
            row += count
        if h in state:
            run_max, run_sum, acc = state[h]
            fade = jnp.exp2(run_max - new_max)
            state[h] = (new_max, run_sum * fade + part_sum, acc * fade + part)
        else:
            state[h] = (new_max, part_sum, part)
    for h in range(heads):
        run_max, run_sum, acc = state[h]
        if last:
            outs[0][:, at(h)] = (acc / run_sum).T.astype(jnp.bfloat16)
        else:
            outs[0][h], outs[1][h], outs[2][at(h), :] = run_max, run_sum, acc


def attend(queries, groups, state, last, block=1, part=(0, 1)):
    rows, all_heads = sum(q.shape[0] for q in queries), queries[0].shape[1] // HEAD_DIM
    heads = all_heads // part[1]
    width, steps = block * HEAD_DIM, heads // block
    half, base = all_heads // block // 2, part[0] * steps
    first = state is None
    state_specs = [
        pl.BlockSpec((block, 1, rows), lambda h: (h + base, 0, 0)),
        pl.BlockSpec((block, 1, rows), lambda h: (h + base, 0, 0)),
        pl.BlockSpec((width, rows), lambda h: (h + base, 0)),
    ]
    state_shapes = [jax.ShapeDtypeStruct((all_heads, 1, rows), jnp.float32)] * 2
    state_shapes.append(jax.ShapeDtypeStruct((all_heads * HEAD_DIM, rows), jnp.float32))
    tall = lambda a: pl.BlockSpec((a.shape[0], width), lambda h: (0, h + base))
    wide = lambda a: pl.BlockSpec((width, a.shape[1]), lambda h: (h + base, 0))
    operands, in_specs, shape, key_rows = list(queries), [tall(q) for q in queries], [len(queries)], 0
    for keys, values_t in groups:
        widths = []
        for k in keys:
            if not isinstance(k, tuple):
                operands.append(k)
                in_specs.append(tall(k))
                widths.append(1)
            elif part[1] == 2:
                operands.append(k[part[0]])
                in_specs.append(pl.BlockSpec((k[0].shape[0], width), lambda h: (0, h)))
                widths.append(1)
            else:
                operands += k
                in_specs.append(pl.BlockSpec((k[0].shape[0], width), lambda h: (0, jnp.minimum(h, half - 1))))
                in_specs.append(pl.BlockSpec((k[1].shape[0], width), lambda h: (0, jnp.maximum(h - half, 0))))
                widths.append(2)
        operands += values_t
        in_specs += [wide(v) for v in values_t]
        shape.append((tuple(widths), len(values_t)))
        key_rows += sum(v.shape[1] for v in values_t)
    count = len(operands)
    o_shape = jax.ShapeDtypeStruct((rows, heads * HEAD_DIM), jnp.bfloat16)
    return pl.pallas_call(
        functools.partial(attend_kernel, tuple(shape), block, half, first, last),
        grid=(steps,),
        in_specs=in_specs + ([] if first else state_specs),
        out_specs=pl.BlockSpec((rows, width), lambda h: (0, h)) if last else state_specs,
        out_shape=o_shape if last else state_shapes,
        input_output_aliases={} if first or last else {count + j: j for j in range(3)},
        cost_estimate=pl.CostEstimate(
            flops=8 * rows * key_rows * heads * HEAD_DIM,
            bytes_accessed=2 * heads * HEAD_DIM * (rows + 2 * key_rows),
            transcendentals=rows * key_rows * heads,
        ),
        compiler_params=pltpu.CompilerParams(vmem_limit_bytes=62 * 2**20),
    )(*operands, *(state or ()))


def project_kernel(flips, width, ranges, rows_of, x_ref, *refs):
    refs = list(refs)
    take = lambda n: [refs.pop(0) for _ in range(n)]
    count = len(flips)
    w_refs = take(count)
    source = take(1)[0] if rows_of and rows_of[0] is not None else None
    picks = rows_of[1] if rows_of else []
    o_refs, pick_refs = take(count), take(len(picks))
    ring, sems = take(2)
    stage = take(1)[0] if source is not None else None
    pick_sem = take(1)[0] if picks else None
    steps = [(stop - start) // width for start, stop in ranges]
    firsts = [sum(steps[:i]) for i in range(count)]

    def copy(i, step, slot):
        columns = pl.ds(pl.multiple_of(ranges[i][0] + step * width, width), width)
        return pltpu.make_async_copy(w_refs[i].at[:, columns], ring.at[slot], sems.at[slot])

    def fetch(n):
        for i in range(count):
            @pl.when(jnp.logical_and(n >= firsts[i], n < firsts[i] + steps[i]))
            def _():
                copy(i, n - firsts[i], lax.rem(n, 3)).start()

    def pick_copies(inward):
        copies, row = [], 0
        for j, (start, rows) in enumerate(picks):
            if source is None:
                copies.append(pltpu.make_async_copy(x_ref.at[pl.ds(start, rows)], pick_refs[j], pick_sem.at[j]))
                continue
            here = stage.at[pl.ds(row, rows)]
            row += rows
            if inward:
                there = source.at[pl.ds(pl.multiple_of(start(), 128), rows)]
                copies.append(pltpu.make_async_copy(there, here, pick_sem.at[j]))
            else:
                copies.append(pltpu.make_async_copy(here, pick_refs[j], pick_sem.at[j]))
        return copies

    fetch(jnp.int32(0))
    fetch(jnp.int32(1))
    for c in pick_copies(True):
        c.start()
    for i in range(count):
        def step(j, carry, i=i):
            n = firsts[i] + j
            slot = lax.rem(n, 3)
            fetch(n + 2)
            copy(i, j, slot).wait()
            block = jnp.dot(x_ref[...], ring[slot], preferred_element_type=jnp.float32)
            columns = pl.ds(pl.multiple_of(j * width, width), width)
            if flips[i]:
                o_refs[i][columns, :] = block.T.astype(jnp.bfloat16)
            else:
                o_refs[i][:, columns] = block.astype(jnp.bfloat16)
            return carry

        lax.fori_loop(0, steps[i], step, 0)
        if source is not None and i == 0:
            for inward, outward in zip(pick_copies(True), pick_copies(False)):
                inward.wait()
                outward.start()
    for c in pick_copies(False):
        c.wait()


def project(x, weights, flips, ranges=None, rows_of=None, width=512):
    rows, depth = x.shape
    ranges = ranges or [(0, w.shape[1]) for w in weights]
    counts = [stop - start for start, stop in ranges]
    shapes = [(c, rows) if f else (rows, c) for c, f in zip(counts, flips)]
    source, picks = rows_of or (None, [])
    any_spec, vmem_spec = pl.BlockSpec(memory_space=pl.ANY), pl.BlockSpec(memory_space=pltpu.VMEM)
    shapes += [(n, (x if source is None else source).shape[1]) for _, n in picks]
    scratch = [pltpu.VMEM((3, depth, width), jnp.bfloat16), pltpu.SemaphoreType.DMA((3,))]
    if source is not None:
        scratch.append(pltpu.VMEM((sum(n for _, n in picks), source.shape[1]), jnp.bfloat16))
    if picks:
        scratch.append(pltpu.SemaphoreType.DMA((len(picks),)))
    static = None if not picks else ('source' if source is not None else None, tuple(picks))
    return pl.pallas_call(
        functools.partial(project_kernel, tuple(flips), width, tuple(ranges), static),
        in_specs=[vmem_spec] + [any_spec] * (len(weights) + (source is not None)),
        out_specs=[vmem_spec] * len(weights) + [any_spec] * len(picks),
        out_shape=[jax.ShapeDtypeStruct(s, jnp.bfloat16) for s in shapes],
        scratch_shapes=scratch,
        cost_estimate=pl.CostEstimate(
            flops=2 * rows * depth * sum(counts),
            bytes_accessed=2 * depth * sum(counts),
            transcendentals=0,
        ),
        compiler_params=pltpu.CompilerParams(vmem_limit_bytes=62 * 2**20),
    )(x, *weights, *(() if source is None else (source,)))


def fold_kernel(depths, lhs_count, has_base, first_unit, *refs):
    lhs_refs, refs = refs[:lhs_count], refs[lhs_count:]
    lhs_ref, refs = refs[-1], refs[:-1]

    @pl.when(pl.program_id(0) == 0)
    def _():
        column = 0
        for ref in lhs_refs:
            lhs_ref[:, column:column + ref.shape[1]] = ref[...]
            column += ref.shape[1]

    if len(depths) == 1:
        left, right = lhs_ref[...], refs[0][...]
    else:
        starts = [pl.multiple_of(first_unit[i] * 128, 128) for i in range(len(depths))]
        left = jnp.concatenate([lhs_ref[:, pl.ds(s, d)] for s, d in zip(starts, depths)], axis=1)
        right = jnp.concatenate([refs[i][...] for i in range(len(depths))], axis=0)
    total = jnp.dot(left, right, preferred_element_type=jnp.float32)
    if has_base:
        total += refs[len(depths)][...]
    refs[-1][...] = total.astype(refs[-1].dtype)


def fold(lhs, pieces, units, base, dtype, part=(0, 1), width=512):
    rows, columns = lhs[0].shape[0], pieces[0].shape[1]
    depths = tuple(p.shape[0] for p in pieces)
    steps = columns // width // part[1]
    first = part[0] * steps
    here = lambda j, r: (0, j + first)
    out_spec = pl.BlockSpec((rows, width), here)
    inputs = [*lhs, *pieces] + ([] if base is None else [base])
    return pl.pallas_call(
        functools.partial(fold_kernel, depths, len(lhs), base is not None),
        grid_spec=pltpu.PrefetchScalarGridSpec(
            num_scalar_prefetch=1,
            grid=(steps,),
            in_specs=[pl.BlockSpec(a.shape, lambda j, r: (0, 0)) for a in lhs]
            + [pl.BlockSpec((d, width), here) for d in depths]
            + ([] if base is None else [pl.BlockSpec((rows, width), here)]),
            out_specs=out_spec,
            scratch_shapes=[pltpu.VMEM((rows, sum(a.shape[1] for a in lhs)), jnp.bfloat16)],
        ),
        out_shape=jax.ShapeDtypeStruct((rows, columns), dtype),
        input_output_aliases={len(inputs): 0} if part[1] > 1 else {},
        cost_estimate=pl.CostEstimate(
            flops=2 * rows * steps * width * sum(depths),
            bytes_accessed=2 * steps * width * sum(depths),
            transcendentals=0,
        ),
        compiler_params=pltpu.CompilerParams(vmem_limit_bytes=62 * 2**20),
    )(jnp.stack(units).astype(jnp.int32), *inputs)


def after(value, *tokens):
    return lax.optimization_barrier((value, *tokens))[0]


def solution(mesh):
    hp_swap = [(0, 1), (1, 0)]
    x_swap = [(0, 2), (1, 3), (2, 0), (3, 1)]
    core_swap = [(0, 1), (1, 0), (2, 3), (3, 2)]

    def device_fn(x_own, w_q, w_k, w_v, w_o):
        sp = lax.axis_index('sp')
        chip, core = sp // 2, sp % 2
        half = x_own.shape[0] // 2
        over_y = lambda a: lax.ppermute(a, 'hp', hp_swap)
        over_x = lambda a: lax.ppermute(a, 'sp', x_swap)
        over_core = lambda a: lax.ppermute(a, 'sp', core_swap)

        def proj(x, weights, flips, ranges=None, rows_of=None):
            return project(x, weights, flips, ranges, rows_of)

        unit_a = lambda chip_, core_: chip_ * 10 + core_ * 3
        unit_b = lambda core_: 6 + core_ * 2

        middle = w_k.shape[1] // 2
        x_f0 = over_y(x_own[:half])
        k_oa, x_half = proj(x_own, [w_k], [False], [(0, middle)], (None, [(half, half)]))
        k_xoa = over_x(k_oa)
        (k_ob,) = proj(after(x_own, k_oa), [w_k], [False], [(middle, 2 * middle)])
        k_xob = over_x(k_ob)
        x_f1 = over_y(x_half)
        first_a = lambda: unit_a(lax.axis_index('sp') // 2, lax.axis_index('sp') % 2) * 128
        first_b = lambda: unit_b(lax.axis_index('sp') % 2) * 128
        v_o, q_o, rows_a, rows_b = proj(
            after(x_own, k_ob), [w_v, w_q], [True, False], None, (w_o, [(first_a, 384), (first_b, 256)])
        )
        v_xo = over_x(v_o)
        wa = over_y(rows_a)
        wb = over_y(after(rows_b, rows_a))
        k_soa, k_sob, v_so = over_core(after(k_oa, v_o)), over_core(after(k_ob, v_o)), over_core(v_o)

        all_w, all_f = [w_k, w_v, w_q], [False, True, False]
        k_r0, v_r0, q_r0 = proj(after(x_f0, rows_a, rows_b), all_w, all_f)
        k_xr0, v_xr0 = over_x(k_r0), over_x(v_r0)
        k_sr0, v_sr0 = over_core(k_r0), over_core(v_r0)
        own, own_s = ([(k_oa, k_ob)], [v_o]), ([(k_soa, k_sob)], [v_so])
        state_o = attend([after(q_o, q_r0)], [own, own_s], None, False, 4)

        k_r1, v_r1, q_r1 = proj(after(x_f1, state_o[0]), all_w, all_f)
        k_xr1, v_xr1 = over_x(k_r1), over_x(v_r1)
        k_sr1, v_sr1 = over_core(k_r1), over_core(v_r1)
        k_sxoa, k_sxob = over_core(after(k_xoa, q_r0)), over_core(after(k_xob, q_r0))
        v_sxo = over_core(after(v_xo, v_r1))
        far, far_s = ([k_r0, k_r1], [v_r0, v_r1]), ([k_sr0, k_sr1], [v_sr0, v_sr1])
        xo, xo_s = ([(k_xoa, k_xob)], [v_xo]), ([(k_sxoa, k_sxob)], [v_sxo])
        state_r = attend([q_r0, q_r1], [own, own_s, far], None, False, 2)
        state_o = attend([after(q_o, state_r[0])], [far, far_s, xo, xo_s], state_o, False, 2)
        k_sxr0, v_sxr0 = over_core(after(k_xr0, state_o[0])), over_core(after(v_xr0, state_o[0]))
        late = ([k_xr0, k_sxr0], [v_xr0, v_sxr0])
        state_r = attend([after(q_r0, state_o[0]), q_r1], [far_s, xo, xo_s], state_r, False, 2)
        wx = over_x(after(wa, state_o[0]))
        wa_s = over_core(after(wa, state_o[0]))

        k_sxr1, v_sxr1 = over_core(after(k_xr1, state_r[0])), over_core(after(v_xr1, state_r[0]))
        latest = ([k_xr1, k_sxr1], [v_xr1, v_sxr1])
        o_ra = attend([q_r0, q_r1], [late, latest], state_r, True, 4, (0, 2))
        o_fa = over_y(o_ra)
        o_rb = attend([after(q_r0, o_ra), q_r1], [late, latest], state_r, True, 4, (1, 2))
        o_fb = over_y(o_rb)
        wb_s = over_core(after(wb, o_rb))
        o_own = attend([after(q_o, o_rb)], [late, latest], state_o, True, 4)
        total = fold([o_own], [w_o], [sp * 0], None, jnp.float32)
        wx_s = over_core(after(wx, total))
        units = [unit_a(chip, core), unit_a(chip, 1 - core), unit_b(core), unit_b(1 - core)]
        units += [unit_a(1 - chip, core), unit_a(1 - chip, 1 - core)]
        return fold([o_fa, after(o_fb, wx)], [wa, wa_s, wb, wb_s, wx, wx_s], units, total, jnp.bfloat16)

    seq_spec = P(('dp', 'sp', 'hp'), None)
    in_specs = (seq_spec, P(None, 'hp'), P(None, 'hp'), P(None, 'hp'), P('hp', None))
    return jax.shard_map(device_fn, mesh=mesh, in_specs=in_specs, out_specs=seq_spec, check_vma=False)
```

```python
import functools
import math

import jax
import jax.numpy as jnp
from jax import lax
from jax.experimental import pallas as pl
from jax.experimental.pallas import tpu as pltpu
from jax.sharding import PartitionSpec as P


HEAD_DIM = 128
EXP2_SCALE = math.log2(math.e) / math.sqrt(HEAD_DIM)


def attend_kernel(shape, heads, split, first, last, scalars, *refs):
    refs = list(refs)
    take = lambda n: [refs.pop(0) for _ in range(n)]
    take(scalars)
    q_refs = take(shape[0])
    groups = [([take(k) for k in widths], take(v)) for widths, v in shape[1:]]
    state_in = None if first else take(3)
    outs = refs
    at = lambda h: slice(h * HEAD_DIM, (h + 1) * HEAD_DIM)
    queries = [jnp.concatenate([r[:, at(h)] for r in q_refs], axis=0) for h in range(heads)]
    low = pl.program_id(0) < split

    def keys_of(piece, h):
        if len(piece) == 1:
            return piece[0][:, at(h)]
        return jnp.where(low, piece[0][:, at(h)], piece[1][:, at(h)])

    def scores_of(h, g):
        parts = [
            lax.dot_general(keys_of(k, h), queries[h], (((1,), (1,)), ((), ())), preferred_element_type=jnp.float32)
            for k in groups[g][0]
        ]
        return parts[0] if len(parts) == 1 else jnp.concatenate(parts, axis=0)

    items = [(h, g) for g in range(len(groups)) for h in range(heads)]
    depth = 2
    state = {} if first else {h: (state_in[0][h], state_in[1][h], state_in[2][at(h), :]) for h in range(heads)}
    ahead = [scores_of(*items[i]) for i in range(min(depth, len(items)))]
    for i, (h, g) in enumerate(items):
        if i + depth < len(items):
            ahead.append(scores_of(*items[i + depth]))
        scores = ahead.pop(0)
        new_max = jnp.max(scores, axis=0, keepdims=True) * EXP2_SCALE
        if h in state:
            new_max = jnp.maximum(state[h][0], new_max)
        probs = jnp.exp2(scores * EXP2_SCALE - new_max)
        part_sum = jnp.sum(probs, axis=0, keepdims=True)
        probs = probs.astype(jnp.bfloat16)
        part, row = None, 0
        for v in groups[g][1]:
            count = v.shape[1]
            piece = jnp.dot(v[at(h), :], probs[row:row + count], preferred_element_type=jnp.float32)
            part = piece if part is None else part + piece
            row += count
        if h in state:
            run_max, run_sum, acc = state[h]
            fade = jnp.exp2(run_max - new_max)
            state[h] = (new_max, run_sum * fade + part_sum, acc * fade + part)
        else:
            state[h] = (new_max, part_sum, part)
    for h in range(heads):
        run_max, run_sum, acc = state[h]
        if last:
            outs[0][:, at(h)] = (acc / run_sum).T.astype(jnp.bfloat16)
        else:
            outs[0][h], outs[1][h], outs[2][at(h), :] = run_max, run_sum, acc


def attend(queries, groups, state, last, block=1, part=None):
    rows, all_heads = sum(q.shape[0] for q in queries), queries[0].shape[1] // HEAD_DIM
    heads = all_heads if part is None else all_heads // 2
    width, steps = block * HEAD_DIM, heads // block
    split, offset = 0, () if part is None else (jnp.full((1,), part * steps, jnp.int32),)
    shift = lambda h, o: h + o[0][0] if o else h
    spec = lambda block, index: pl.BlockSpec(block, lambda h, *o: index(h, shift(h, o)))
    first = state is None
    state_specs = [
        spec((block, 1, rows), lambda h, g: (g, 0, 0)),
        spec((block, 1, rows), lambda h, g: (g, 0, 0)),
        spec((width, rows), lambda h, g: (g, 0)),
    ]
    state_shapes = [jax.ShapeDtypeStruct((all_heads, 1, rows), jnp.float32)] * 2
    state_shapes.append(jax.ShapeDtypeStruct((all_heads * HEAD_DIM, rows), jnp.float32))
    tall = lambda a: spec((a.shape[0], width), lambda h, g: (0, g))
    wide = lambda a: spec((width, a.shape[1]), lambda h, g: (g, 0))
    operands, in_specs, shape, key_rows = list(queries), [tall(q) for q in queries], [len(queries)], 0
    for keys, values_t in groups:
        widths = []
        for k in keys:
            if not isinstance(k, tuple):
                operands.append(k)
                in_specs.append(tall(k))
                widths.append(1)
            else:
                split = k[0].shape[1] // width
                operands += k
                in_specs.append(spec((k[0].shape[0], width), lambda h, g, s=split: (0, jnp.minimum(h, s - 1))))
                in_specs.append(spec((k[1].shape[0], width), lambda h, g, s=split: (0, jnp.maximum(h - s, 0))))
                widths.append(2)
        operands += values_t
        in_specs += [wide(v) for v in values_t]
        shape.append((tuple(widths), len(values_t)))
        key_rows += sum(v.shape[1] for v in values_t)
    count = len(operands)
    o_shape = jax.ShapeDtypeStruct((rows, heads * HEAD_DIM), jnp.bfloat16)
    return pl.pallas_call(
        functools.partial(attend_kernel, tuple(shape), block, split, first, last, len(offset)),
        grid_spec=pltpu.PrefetchScalarGridSpec(
            num_scalar_prefetch=len(offset),
            grid=(steps,),
            in_specs=in_specs + ([] if first else state_specs),
            out_specs=spec((rows, width), lambda h, g: (0, h)) if last else state_specs,
        ),
        out_shape=o_shape if last else state_shapes,
        input_output_aliases={} if first or last else {len(offset) + count + j: j for j in range(3)},
        cost_estimate=pl.CostEstimate(
            flops=8 * rows * key_rows * heads * HEAD_DIM,
            bytes_accessed=2 * heads * HEAD_DIM * (rows + 2 * key_rows),
            transcendentals=rows * key_rows * heads,
        ),
        compiler_params=pltpu.CompilerParams(vmem_limit_bytes=62 * 2**20),
    )(*offset, *operands, *(state or ()))


def project_kernel(flips, width, ranges, rows_of, x_ref, *refs):
    refs = list(refs)
    take = lambda n: [refs.pop(0) for _ in range(n)]
    count = len(flips)
    w_refs = take(count)
    source = take(1)[0] if rows_of and rows_of[0] is not None else None
    picks = rows_of[1] if rows_of else []
    o_refs, pick_refs = take(count), take(len(picks))
    ring, sems = take(2)
    stage = take(1)[0] if source is not None else None
    pick_sem = take(1)[0] if picks else None
    steps = [(stop - start) // width for start, stop in ranges]
    firsts = [sum(steps[:i]) for i in range(count)]

    def copy(i, step, slot):
        columns = pl.ds(pl.multiple_of(ranges[i][0] + step * width, width), width)
        return pltpu.make_async_copy(w_refs[i].at[:, columns], ring.at[slot], sems.at[slot])

    def fetch(n):
        for i in range(count):
            @pl.when(jnp.logical_and(n >= firsts[i], n < firsts[i] + steps[i]))
            def _():
                copy(i, n - firsts[i], lax.rem(n, 3)).start()

    def pick_copies(inward):
        copies, row = [], 0
        for j, (start, rows) in enumerate(picks):
            if source is None:
                copies.append(pltpu.make_async_copy(x_ref.at[pl.ds(start, rows)], pick_refs[j], pick_sem.at[j]))
                continue
            here = stage.at[pl.ds(row, rows)]
            row += rows
            if inward:
                there = source.at[pl.ds(pl.multiple_of(start(), 128), rows)]
                copies.append(pltpu.make_async_copy(there, here, pick_sem.at[j]))
            else:
                copies.append(pltpu.make_async_copy(here, pick_refs[j], pick_sem.at[j]))
        return copies

    fetch(jnp.int32(0))
    fetch(jnp.int32(1))
    for c in pick_copies(True):
        c.start()
    for i in range(count):
        def step(j, carry, i=i):
            n = firsts[i] + j
            slot = lax.rem(n, 3)
            fetch(n + 2)
            copy(i, j, slot).wait()
            block = jnp.dot(x_ref[...], ring[slot], preferred_element_type=jnp.float32)
            columns = pl.ds(pl.multiple_of(j * width, width), width)
            if flips[i]:
                o_refs[i][columns, :] = block.T.astype(jnp.bfloat16)
            else:
                o_refs[i][:, columns] = block.astype(jnp.bfloat16)
            return carry

        lax.fori_loop(0, steps[i], step, 0)
        if source is not None and i == 0:
            for inward, outward in zip(pick_copies(True), pick_copies(False)):
                inward.wait()
                outward.start()
    for c in pick_copies(False):
        c.wait()


def project(x, weights, flips, ranges=None, rows_of=None, width=512):
    rows, depth = x.shape
    ranges = ranges or [(0, w.shape[1]) for w in weights]
    counts = [stop - start for start, stop in ranges]
    shapes = [(c, rows) if f else (rows, c) for c, f in zip(counts, flips)]
    source, picks = rows_of or (None, [])
    any_spec, vmem_spec = pl.BlockSpec(memory_space=pl.ANY), pl.BlockSpec(memory_space=pltpu.VMEM)
    shapes += [(n, (x if source is None else source).shape[1]) for _, n in picks]
    scratch = [pltpu.VMEM((3, depth, width), jnp.bfloat16), pltpu.SemaphoreType.DMA((3,))]
    if source is not None:
        scratch.append(pltpu.VMEM((sum(n for _, n in picks), source.shape[1]), jnp.bfloat16))
    if picks:
        scratch.append(pltpu.SemaphoreType.DMA((len(picks),)))
    static = None if not picks else ('source' if source is not None else None, tuple(picks))
    return pl.pallas_call(
        functools.partial(project_kernel, tuple(flips), width, tuple(ranges), static),
        in_specs=[vmem_spec] + [any_spec] * (len(weights) + (source is not None)),
        out_specs=[vmem_spec] * len(weights) + [any_spec] * len(picks),
        out_shape=[jax.ShapeDtypeStruct(s, jnp.bfloat16) for s in shapes],
        scratch_shapes=scratch,
        cost_estimate=pl.CostEstimate(
            flops=2 * rows * depth * sum(counts),
            bytes_accessed=2 * depth * sum(counts),
            transcendentals=0,
        ),
        compiler_params=pltpu.CompilerParams(vmem_limit_bytes=62 * 2**20),
    )(x, *weights, *(() if source is None else (source,)))


def fold_kernel(plan, width, has_base, *refs):
    refs = list(refs)
    take = lambda n: [refs.pop(0) for _ in range(n)]
    chip, core = lax.axis_index('sp') // 2, lax.axis_index('sp') % 2
    lhs_refs = take(max(p[1] for p in plan) + 1)
    piece_refs = [take(1 if p[3] is None else 2) for p in plan]
    base_ref = take(1)[0] if has_base else None
    out_ref, left, right, right_sem, outs, out_sem = take(6)
    bases, base_sem = take(2) if has_base else (None, None)
    steps = out_ref.shape[1] // width
    columns = lambda j: pl.ds(pl.multiple_of(j * width, width), width)

    def fetches(j, slot):
        copies, row = [], 0
        for i, (depth, _, _, choice) in enumerate(plan):
            here = right.at[slot, pl.ds(row, depth)]
            versions = [pltpu.make_async_copy(r.at[:, columns(j)], here, right_sem.at[slot, i]) for r in piece_refs[i]]
            copies.append((versions, choice))
            row += depth
        if has_base:
            versions = [pltpu.make_async_copy(base_ref.at[:, columns(j)], bases.at[slot], base_sem.at[slot])]
            copies.append((versions, None))
        return copies

    def fetch(j):
        for versions, choice in fetches(j, lax.rem(j, 3)):
            if choice is None:
                versions[0].start()
                continue
            pl.when(choice(chip, core))(versions[0].start)
            pl.when(jnp.logical_not(choice(chip, core)))(versions[1].start)

    def store(j):
        slot = lax.rem(j, 2)
        return pltpu.make_async_copy(outs.at[slot], out_ref.at[:, columns(j)], out_sem.at[slot])

    fetch(jnp.int32(0))
    fetch(jnp.int32(1))
    column = 0
    for depth, which, start, _ in plan:
        source = lhs_refs[which]
        picked = pl.ds(pl.multiple_of(start(chip, core), 128), depth)
        left[:, column:column + depth] = source[...] if source.shape[1] == depth else source[:, picked]
        column += depth

    def step(j, carry):
        slot = lax.rem(j, 3)

        @pl.when(j + 2 < steps)
        def _():
            fetch(j + 2)

        for versions, _ in fetches(j, slot):
            versions[0].wait()

        total = jnp.dot(left[...], right[slot], preferred_element_type=jnp.float32)
        if has_base:
            total += bases[slot]

        @pl.when(j >= 2)
        def _():
            store(j - 2).wait()

        outs[lax.rem(j, 2)] = total.astype(out_ref.dtype)
        store(j).start()
        return carry

    lax.fori_loop(0, steps, step, 0)
    store(jnp.int32(steps - 2)).wait()
    store(jnp.int32(steps - 1)).wait()


def fold(lhs, pieces, base, dtype, width=512):
    plan, arrays = [], []
    for piece, which, start, choice in pieces:
        versions = piece if isinstance(piece, tuple) else (piece,)
        plan.append((versions[0].shape[0], which, start, choice))
        arrays += versions
    rows, columns, depth = lhs[0].shape[0], arrays[0].shape[1], sum(p[0] for p in plan)
    any_spec, vmem_spec = pl.BlockSpec(memory_space=pl.ANY), pl.BlockSpec(memory_space=pltpu.VMEM)
    scratch = [
        pltpu.VMEM((rows, depth), jnp.bfloat16),
        pltpu.VMEM((3, depth, width), jnp.bfloat16),
        pltpu.SemaphoreType.DMA((3, len(plan))),
        pltpu.VMEM((2, rows, width), dtype),
        pltpu.SemaphoreType.DMA((2,)),
    ]
    if base is not None:
        scratch += [pltpu.VMEM((3, rows, width), jnp.float32), pltpu.SemaphoreType.DMA((3,))]
    return pl.pallas_call(
        functools.partial(fold_kernel, tuple(plan), width, base is not None),
        in_specs=[vmem_spec] * len(lhs) + [any_spec] * (len(arrays) + (base is not None)),
        out_specs=any_spec,
        out_shape=jax.ShapeDtypeStruct((rows, columns), dtype),
        scratch_shapes=scratch,
        cost_estimate=pl.CostEstimate(flops=2 * rows * columns * depth, bytes_accessed=2 * columns * depth, transcendentals=0),
        compiler_params=pltpu.CompilerParams(vmem_limit_bytes=62 * 2**20),
    )(*lhs, *arrays, *(() if base is None else (base,)))


def after(value, *tokens):
    return lax.optimization_barrier((value, *tokens))[0]


def solution(mesh):
    hp_swap = [(0, 1), (1, 0)]
    x_swap = [(0, 2), (1, 3), (2, 0), (3, 1)]
    core_swap = [(0, 1), (1, 0), (2, 3), (3, 2)]

    def device_fn(x_own, w_q, w_k, w_v, w_o):
        sp = lax.axis_index('sp')
        chip = sp // 2
        half = x_own.shape[0] // 2
        over_y = lambda a: lax.ppermute(a, 'hp', hp_swap)
        over_x = lambda a: lax.ppermute(a, 'sp', x_swap)
        over_core = lambda a: lax.ppermute(a, 'sp', core_swap)

        def proj(x, weights, flips, ranges=None, rows_of=None):
            return project(x, weights, flips, ranges, rows_of)

        unit_a = lambda chip_, core_: chip_ * 10 + core_ * 3
        unit_b = lambda core_: 6 + core_ * 2

        middle = w_k.shape[1] // 4
        x_f0 = over_y(x_own[:half])
        k_oa, x_half = proj(x_own, [w_k], [False], [(0, middle)], (None, [(half, half)]))
        k_xoa = over_x(k_oa)
        (k_ob,) = proj(after(x_own, k_oa), [w_k], [False], [(middle, 4 * middle)])
        k_xob = over_x(k_ob)
        x_f1 = over_y(x_half)
        first_a = lambda: unit_a(lax.axis_index('sp') // 2, lax.axis_index('sp') % 2) * 128
        first_a1 = lambda: first_a() + 256
        first_b = lambda: unit_b(lax.axis_index('sp') % 2) * 128
        v_o, q_o, rows_a0, rows_a1, rows_b = proj(
            after(x_own, k_ob), [w_v, w_q], [True, False], None, (w_o, [(first_a, 256), (first_a1, 128), (first_b, 256)])
        )
        v_xo = over_x(v_o)
        wa0, wa1, wb = over_y(rows_a0), over_y(rows_a1), over_y(rows_b)
        k_soa, k_sob, v_so = over_core(after(k_oa, v_o)), over_core(after(k_ob, v_o)), over_core(v_o)

        all_w, all_f = [w_k, w_v, w_q], [False, True, False]
        k_r0, v_r0, q_r0 = proj(after(x_f0, rows_b), all_w, all_f)
        k_xr0, v_xr0 = over_x(k_r0), over_x(v_r0)
        k_sr0, v_sr0 = over_core(k_r0), over_core(v_r0)
        own, own_s = ([(k_oa, k_ob)], [v_o]), ([(k_soa, k_sob)], [v_so])
        state_o = attend([after(q_o, q_r0)], [own, own_s], None, False, 4)

        k_r1, v_r1 = proj(after(x_f1, state_o[0]), [w_k, w_v], [False, True])
        k_xr1, v_xr1 = over_x(k_r1), over_x(v_r1)
        k_sr1, v_sr1 = over_core(k_r1), over_core(v_r1)
        v_sxo = over_core(after(v_xo, v_r1))
        (q_r1,) = proj(after(x_f1, v_r1), [w_q], [False])
        k_sxoa, k_sxob = over_core(after(k_xoa, q_r0)), over_core(after(k_xob, q_r0))
        far, far_s = ([k_r0, k_r1], [v_r0, v_r1]), ([k_sr0, k_sr1], [v_sr0, v_sr1])
        xo, xo_s = ([(k_xoa, k_xob)], [v_xo]), ([(k_sxoa, k_sxob)], [v_sxo])
        state_r = attend([q_r0, q_r1], [own, own_s, far, far_s, xo, xo_s], None, False, 2)
        k_sxr0, v_sxr0 = over_core(after(k_xr0, state_r[0])), over_core(after(v_xr0, state_r[0]))
        late = ([k_xr0, k_sxr0], [v_xr0, v_sxr0])
        state_o = attend([after(q_o, state_r[0])], [far, far_s, xo, xo_s], state_o, False, 2)
        wx0, wx1 = over_x(after(wa0, state_r[0])), over_x(after(wa1, state_o[0]))
        wa0_s, wa1_s = over_core(after(wa0, state_r[0])), over_core(after(wa1, state_o[0]))

        k_sxr1, v_sxr1 = over_core(after(k_xr1, state_o[0])), over_core(after(v_xr1, state_o[0]))
        latest = ([k_xr1, k_sxr1], [v_xr1, v_sxr1])
        o_ra = attend([after(q_r0, state_o[0]), q_r1], [late, latest], state_r, True, 4, chip)
        o_fa = over_y(o_ra)
        o_rb = attend([after(q_r0, o_ra), q_r1], [late, latest], state_r, True, 4, 1 - chip)
        o_fb = over_y(o_rb)
        wb_s = over_core(after(wb, o_rb))
        o_own = attend([after(q_o, o_rb)], [late, latest], state_o, True, 4)
        near = lambda core_of, more: lambda x, c: (x * 2 + core_of(c) * 3 + more) * 128
        away = lambda core_of, more: lambda x, c: ((1 - x) * 2 + core_of(c) * 3 + more) * 128
        same, other, zero = lambda c: c, lambda c: 1 - c, lambda x, c: 0
        pieces = [(w_o, 0, zero, None), (wa0, 1, near(same, 0), None), (wa0_s, 1, near(other, 0), None)]
        pieces += [(wa1, 1, near(same, 2), None), (wa1_s, 1, near(other, 2), None)]
        pieces.append(((wb, wb_s), 1, lambda x, c: (1 - x) * 768, lambda x, c: c == x))
        total = fold([o_own, o_fa], pieces, None, jnp.float32)
        wx0_s = over_core(after(wx0, o_own))
        wx1_s = over_core(after(wx1, total))
        pieces = [((wb, wb_s), 0, lambda x, c: x * 768, lambda x, c: c != x)]
        pieces += [(wx0, 0, away(same, 0), None), (wx0_s, 0, away(other, 0), None)]
        pieces += [(wx1, 0, away(same, 2), None), (wx1_s, 0, away(other, 2), None)]
        return fold([after(o_fb, wx1)], pieces, total, jnp.bfloat16)

    seq_spec = P(('dp', 'sp', 'hp'), None)
    in_specs = (seq_spec, P(None, 'hp'), P(None, 'hp'), P(None, 'hp'), P('hp', None))
    return jax.shard_map(device_fn, mesh=mesh, in_specs=in_specs, out_specs=seq_spec, check_vma=False)
```

```python
import functools
import math

import jax
import jax.numpy as jnp
from jax import lax
from jax.experimental import pallas as pl
from jax.experimental.pallas import tpu as pltpu
from jax.sharding import PartitionSpec as P


HEAD_DIM = 128
EXP2_SCALE = math.log2(math.e) / math.sqrt(HEAD_DIM)
CHUNK = 256
SUM_LIMIT = 2.0**60
ACC_LIMIT = 3.0e38


def attend_kernel(shape, heads, split, first, last, scalars, *refs):
    refs = list(refs)
    take = lambda n: [refs.pop(0) for _ in range(n)]
    take(scalars)
    q_refs = take(shape[0])
    groups = [([take(k) for k in widths], take(v)) for widths, v in shape[1:]]
    state_in = None if first else take(3)
    outs, q_copy = refs[:-1], refs[-1]
    low = pl.program_id(0) < split
    chunks = []
    for pieces, values in groups:
        k_parts = [(p, r) for p in pieces for r in range(0, p[0].shape[0], CHUNK)]
        v_parts = [(v, c) for v in values for c in range(0, v.shape[1], CHUNK)]
        chunks += [k + v for k, v in zip(k_parts, v_parts)]

    def scores_of(chunk, at, query):
        piece, row = chunk[:2]
        keys = piece[0][row:row + CHUNK, at]
        if len(piece) > 1:
            keys = jnp.where(low, keys, piece[1][row:row + CHUNK, at])
        return lax.dot_general(keys, query, (((1,), (1,)), ((), ())), preferred_element_type=jnp.float32)

    def values_of(chunk, at, probs):
        v, column = chunk[2:]
        return jnp.dot(v[at, column:column + CHUNK], probs, preferred_element_type=jnp.float32)

    fixed = [slice(h * HEAD_DIM, (h + 1) * HEAD_DIM) for h in range(heads)]
    queries = [jnp.concatenate([r[:, at] for r in q_refs], axis=0) for at in fixed]
    items = [(h, c) for c in range(len(chunks)) for h in range(heads)]
    depth = 2
    state = {} if first else {h: (state_in[0][h], state_in[1][h], state_in[2][fixed[h], :]) for h in range(heads)}
    score = lambda h, c: scores_of(chunks[c], fixed[h], queries[h])
    ahead = [score(*item) for item in items[:depth]]
    for i, (h, c) in enumerate(items):
        if i + depth < len(items):
            ahead.append(score(*items[i + depth]))
        scores = ahead.pop(0)
        shift = state[h][0] if h in state else jnp.max(scores, axis=0, keepdims=True) * EXP2_SCALE
        probs = jnp.exp2(scores * EXP2_SCALE - shift)
        part_sum = jnp.sum(probs, axis=0, keepdims=True)
        part = values_of(chunks[c], fixed[h], probs.astype(jnp.bfloat16))
        state[h] = (shift, state[h][1] + part_sum, state[h][2] + part) if h in state else (shift, part_sum, part)

    fine = None
    for h in range(heads):
        shift, run_sum, acc = state[h]
        good = jnp.logical_and(jnp.max(run_sum) < SUM_LIMIT, jnp.max(jnp.abs(acc)) < ACC_LIMIT)
        fine = good if fine is None else jnp.logical_and(fine, good)
        if last:
            outs[0][:, fixed[h]] = (acc / run_sum).T.astype(jnp.bfloat16)
        else:
            outs[0][h], outs[1][h], outs[2][fixed[h], :] = shift, run_sum, acc

    @pl.when(jnp.logical_not(fine))
    def _():
        row = 0
        for r in q_refs:
            q_copy[row:row + r.shape[0], :] = r[...]
            row += r.shape[0]

        def redo(n, carry):
            h = n // (row // HEAD_DIM)
            at = pl.ds(pl.multiple_of(h * HEAD_DIM, HEAD_DIM), HEAD_DIM)
            spot = pl.ds(pl.multiple_of((n % (row // HEAD_DIM)) * HEAD_DIM, HEAD_DIM), HEAD_DIM)
            query = q_copy[spot, at]
            if first:
                run_max = jnp.full((1, HEAD_DIM), -jnp.inf, jnp.float32)
                run_sum, acc = jnp.zeros((1, HEAD_DIM), jnp.float32), jnp.zeros((HEAD_DIM, HEAD_DIM), jnp.float32)
            else:
                run_max, run_sum, acc = state_in[0][h, :, spot], state_in[1][h, :, spot], state_in[2][at, spot]
            for chunk in chunks:
                scaled = scores_of(chunk, at, query) * EXP2_SCALE
                new_max = jnp.maximum(run_max, jnp.max(scaled, axis=0, keepdims=True))
                fade = jnp.exp2(run_max - new_max)
                probs = jnp.exp2(scaled - new_max)
                run_sum = run_sum * fade + jnp.sum(probs, axis=0, keepdims=True)
                acc = acc * fade + values_of(chunk, at, probs.astype(jnp.bfloat16))
                run_max = new_max
            if last:
                outs[0][spot, at] = (acc / run_sum).T.astype(jnp.bfloat16)
            else:
                outs[0][h, :, spot], outs[1][h, :, spot], outs[2][at, spot] = run_max, run_sum, acc
            return carry

        lax.fori_loop(0, heads * (row // HEAD_DIM), redo, 0)


def attend(queries, groups, state, last, block=1, part=None):
    rows, all_heads = sum(q.shape[0] for q in queries), queries[0].shape[1] // HEAD_DIM
    heads = all_heads if part is None else all_heads // 2
    width, steps = block * HEAD_DIM, heads // block
    split, offset = 0, () if part is None else (jnp.full((1,), part * steps, jnp.int32),)
    shift = lambda h, o: h + o[0][0] if o else h
    spec = lambda block, index: pl.BlockSpec(block, lambda h, *o: index(h, shift(h, o)))
    first = state is None
    state_specs = [
        spec((block, 1, rows), lambda h, g: (g, 0, 0)),
        spec((block, 1, rows), lambda h, g: (g, 0, 0)),
        spec((width, rows), lambda h, g: (g, 0)),
    ]
    state_shapes = [jax.ShapeDtypeStruct((all_heads, 1, rows), jnp.float32)] * 2
    state_shapes.append(jax.ShapeDtypeStruct((all_heads * HEAD_DIM, rows), jnp.float32))
    tall = lambda a: spec((a.shape[0], width), lambda h, g: (0, g))
    wide = lambda a: spec((width, a.shape[1]), lambda h, g: (g, 0))
    operands, in_specs, shape, key_rows = list(queries), [tall(q) for q in queries], [len(queries)], 0
    for keys, values_t in groups:
        widths = []
        for k in keys:
            if not isinstance(k, tuple):
                operands.append(k)
                in_specs.append(tall(k))
                widths.append(1)
            else:
                split = k[0].shape[1] // width
                operands += k
                in_specs.append(spec((k[0].shape[0], width), lambda h, g, s=split: (0, jnp.minimum(h, s - 1))))
                in_specs.append(spec((k[1].shape[0], width), lambda h, g, s=split: (0, jnp.maximum(h - s, 0))))
                widths.append(2)
        operands += values_t
        in_specs += [wide(v) for v in values_t]
        shape.append((tuple(widths), len(values_t)))
        key_rows += sum(v.shape[1] for v in values_t)
    count = len(operands)
    o_shape = jax.ShapeDtypeStruct((rows, heads * HEAD_DIM), jnp.bfloat16)
    return pl.pallas_call(
        functools.partial(attend_kernel, tuple(shape), block, split, first, last, len(offset)),
        grid_spec=pltpu.PrefetchScalarGridSpec(
            num_scalar_prefetch=len(offset),
            grid=(steps,),
            in_specs=in_specs + ([] if first else state_specs),
            out_specs=spec((rows, width), lambda h, g: (0, h)) if last else state_specs,
            scratch_shapes=[pltpu.VMEM((rows, width), jnp.bfloat16)],
        ),
        out_shape=o_shape if last else state_shapes,
        input_output_aliases={} if first or last else {len(offset) + count + j: j for j in range(3)},
        cost_estimate=pl.CostEstimate(
            flops=8 * rows * key_rows * heads * HEAD_DIM,
            bytes_accessed=2 * heads * HEAD_DIM * (rows + 2 * key_rows),
            transcendentals=rows * key_rows * heads,
        ),
        compiler_params=pltpu.CompilerParams(vmem_limit_bytes=62 * 2**20),
    )(*offset, *operands, *(state or ()))


def project_kernel(flips, width, ranges, rows_of, x_ref, *refs):
    refs = list(refs)
    take = lambda n: [refs.pop(0) for _ in range(n)]
    count = len(flips)
    w_refs = take(count)
    source = take(1)[0] if rows_of and rows_of[0] is not None else None
    picks = rows_of[1] if rows_of else []
    o_refs, pick_refs = take(count), take(len(picks))
    ring, sems = take(2)
    stage = take(1)[0] if source is not None else None
    pick_sem = take(1)[0] if picks else None
    steps = [(stop - start) // width for start, stop in ranges]
    firsts = [sum(steps[:i]) for i in range(count)]

    def copy(i, step, slot):
        columns = pl.ds(pl.multiple_of(ranges[i][0] + step * width, width), width)
        return pltpu.make_async_copy(w_refs[i].at[:, columns], ring.at[slot], sems.at[slot])

    def fetch(n):
        for i in range(count):
            @pl.when(jnp.logical_and(n >= firsts[i], n < firsts[i] + steps[i]))
            def _():
                copy(i, n - firsts[i], lax.rem(n, 3)).start()

    def pick_copies(inward):
        copies, row = [], 0
        for j, (start, rows) in enumerate(picks):
            if source is None:
                copies.append(pltpu.make_async_copy(x_ref.at[pl.ds(start, rows)], pick_refs[j], pick_sem.at[j]))
                continue
            here = stage.at[pl.ds(row, rows)]
            row += rows
            if inward:
                there = source.at[pl.ds(pl.multiple_of(start(), 128), rows)]
                copies.append(pltpu.make_async_copy(there, here, pick_sem.at[j]))
            else:
                copies.append(pltpu.make_async_copy(here, pick_refs[j], pick_sem.at[j]))
        return copies

    fetch(jnp.int32(0))
    fetch(jnp.int32(1))
    for c in pick_copies(True):
        c.start()
    for i in range(count):
        def step(j, carry, i=i):
            n = firsts[i] + j
            slot = lax.rem(n, 3)
            fetch(n + 2)
            copy(i, j, slot).wait()
            block = jnp.dot(x_ref[...], ring[slot], preferred_element_type=jnp.float32)
            columns = pl.ds(pl.multiple_of(j * width, width), width)
            if flips[i]:
                o_refs[i][columns, :] = block.T.astype(jnp.bfloat16)
            else:
                o_refs[i][:, columns] = block.astype(jnp.bfloat16)
            return carry

        lax.fori_loop(0, steps[i], step, 0)
        if source is not None and i == 0:
            for inward, outward in zip(pick_copies(True), pick_copies(False)):
                inward.wait()
                outward.start()
    for c in pick_copies(False):
        c.wait()


def project(x, weights, flips, ranges=None, rows_of=None, width=512):
    rows, depth = x.shape
    ranges = ranges or [(0, w.shape[1]) for w in weights]
    counts = [stop - start for start, stop in ranges]
    shapes = [(c, rows) if f else (rows, c) for c, f in zip(counts, flips)]
    source, picks = rows_of or (None, [])
    any_spec, vmem_spec = pl.BlockSpec(memory_space=pl.ANY), pl.BlockSpec(memory_space=pltpu.VMEM)
    shapes += [(n, (x if source is None else source).shape[1]) for _, n in picks]
    scratch = [pltpu.VMEM((3, depth, width), jnp.bfloat16), pltpu.SemaphoreType.DMA((3,))]
    if source is not None:
        scratch.append(pltpu.VMEM((sum(n for _, n in picks), source.shape[1]), jnp.bfloat16))
    if picks:
        scratch.append(pltpu.SemaphoreType.DMA((len(picks),)))
    static = None if not picks else ('source' if source is not None else None, tuple(picks))
    return pl.pallas_call(
        functools.partial(project_kernel, tuple(flips), width, tuple(ranges), static),
        in_specs=[vmem_spec] + [any_spec] * (len(weights) + (source is not None)),
        out_specs=[vmem_spec] * len(weights) + [any_spec] * len(picks),
        out_shape=[jax.ShapeDtypeStruct(s, jnp.bfloat16) for s in shapes],
        scratch_shapes=scratch,
        cost_estimate=pl.CostEstimate(
            flops=2 * rows * depth * sum(counts),
            bytes_accessed=2 * depth * sum(counts),
            transcendentals=0,
        ),
        compiler_params=pltpu.CompilerParams(vmem_limit_bytes=62 * 2**20),
    )(x, *weights, *(() if source is None else (source,)))


def fold_kernel(plan, width, has_base, *refs):
    refs = list(refs)
    take = lambda n: [refs.pop(0) for _ in range(n)]
    chip, core = lax.axis_index('sp') // 2, lax.axis_index('sp') % 2
    lhs_refs = take(max(p[1] for p in plan) + 1)
    piece_refs = [take(1 if p[3] is None else 2) for p in plan]
    base_ref = take(1)[0] if has_base else None
    out_ref, left, right, right_sem, outs, out_sem = take(6)
    bases, base_sem = take(2) if has_base else (None, None)
    steps = out_ref.shape[1] // width
    columns = lambda j: pl.ds(pl.multiple_of(j * width, width), width)

    def fetches(j, slot):
        copies, row = [], 0
        for i, (depth, _, _, choice) in enumerate(plan):
            here = right.at[slot, pl.ds(row, depth)]
            versions = [pltpu.make_async_copy(r.at[:, columns(j)], here, right_sem.at[slot, i]) for r in piece_refs[i]]
            copies.append((versions, choice))
            row += depth
        if has_base:
            versions = [pltpu.make_async_copy(base_ref.at[:, columns(j)], bases.at[slot], base_sem.at[slot])]
            copies.append((versions, None))
        return copies

    def fetch(j):
        for versions, choice in fetches(j, lax.rem(j, 3)):
            if choice is None:
                versions[0].start()
                continue
            pl.when(choice(chip, core))(versions[0].start)
            pl.when(jnp.logical_not(choice(chip, core)))(versions[1].start)

    def store(j):
        slot = lax.rem(j, 2)
        return pltpu.make_async_copy(outs.at[slot], out_ref.at[:, columns(j)], out_sem.at[slot])

    fetch(jnp.int32(0))
    fetch(jnp.int32(1))
    column = 0
    for depth, which, start, _ in plan:
        source = lhs_refs[which]
        picked = pl.ds(pl.multiple_of(start(chip, core), 128), depth)
        left[:, column:column + depth] = source[...] if source.shape[1] == depth else source[:, picked]
        column += depth

    def step(j, carry):
        slot = lax.rem(j, 3)

        @pl.when(j + 2 < steps)
        def _():
            fetch(j + 2)

        for versions, _ in fetches(j, slot):
            versions[0].wait()

        total = jnp.dot(left[...], right[slot], preferred_element_type=jnp.float32)
        if has_base:
            total += bases[slot]

        @pl.when(j >= 2)
        def _():
            store(j - 2).wait()

        outs[lax.rem(j, 2)] = total.astype(out_ref.dtype)
        store(j).start()
        return carry

    lax.fori_loop(0, steps, step, 0)
    store(jnp.int32(steps - 2)).wait()
    store(jnp.int32(steps - 1)).wait()


def fold(lhs, pieces, base, dtype, width=512):
    plan, arrays = [], []
    for piece, which, start, choice in pieces:
        versions = piece if isinstance(piece, tuple) else (piece,)
        plan.append((versions[0].shape[0], which, start, choice))
        arrays += versions
    rows, columns, depth = lhs[0].shape[0], arrays[0].shape[1], sum(p[0] for p in plan)
    any_spec, vmem_spec = pl.BlockSpec(memory_space=pl.ANY), pl.BlockSpec(memory_space=pltpu.VMEM)
    scratch = [
        pltpu.VMEM((rows, depth), jnp.bfloat16),
        pltpu.VMEM((3, depth, width), jnp.bfloat16),
        pltpu.SemaphoreType.DMA((3, len(plan))),
        pltpu.VMEM((2, rows, width), dtype),
        pltpu.SemaphoreType.DMA((2,)),
    ]
    if base is not None:
        scratch += [pltpu.VMEM((3, rows, width), jnp.float32), pltpu.SemaphoreType.DMA((3,))]
    return pl.pallas_call(
        functools.partial(fold_kernel, tuple(plan), width, base is not None),
        in_specs=[vmem_spec] * len(lhs) + [any_spec] * (len(arrays) + (base is not None)),
        out_specs=any_spec,
        out_shape=jax.ShapeDtypeStruct((rows, columns), dtype),
        scratch_shapes=scratch,
        cost_estimate=pl.CostEstimate(flops=2 * rows * columns * depth, bytes_accessed=2 * columns * depth, transcendentals=0),
        compiler_params=pltpu.CompilerParams(vmem_limit_bytes=62 * 2**20),
    )(*lhs, *arrays, *(() if base is None else (base,)))


def after(value, *tokens):
    return lax.optimization_barrier((value, *tokens))[0]


def solution(mesh):
    hp_swap = [(0, 1), (1, 0)]
    x_swap = [(0, 2), (1, 3), (2, 0), (3, 1)]
    core_swap = [(0, 1), (1, 0), (2, 3), (3, 2)]

    def device_fn(x_own, w_q, w_k, w_v, w_o):
        sp = lax.axis_index('sp')
        chip = sp // 2
        half = x_own.shape[0] // 2
        over_y = lambda a: lax.ppermute(a, 'hp', hp_swap)
        over_x = lambda a: lax.ppermute(a, 'sp', x_swap)
        over_core = lambda a: lax.ppermute(a, 'sp', core_swap)

        def proj(x, weights, flips, ranges=None, rows_of=None, width=512):
            return project(x, weights, flips, ranges, rows_of, width)

        unit_a = lambda chip_, core_: chip_ * 10 + core_ * 3
        unit_b = lambda core_: 6 + core_ * 2

        middle = w_k.shape[1] // 2
        k_oa, x_half0, x_half = proj(x_own, [w_k], [False], [(0, middle)], (None, [(0, half), (half, half)]), 256)
        k_xoa = over_x(k_oa)
        x_f0 = over_y(x_half0)
        (k_ob,) = proj(after(x_own, k_oa), [w_k], [False], [(middle, 2 * middle)])
        k_xob = over_x(k_ob)
        x_f1 = over_y(x_half)
        first_a = lambda: unit_a(lax.axis_index('sp') // 2, lax.axis_index('sp') % 2) * 128
        first_a1 = lambda: first_a() + 256
        first_b = lambda: unit_b(lax.axis_index('sp') % 2) * 128
        v_o, q_o, rows_a0, rows_a1, rows_b = proj(
            after(x_own, k_ob), [w_v, w_q], [True, False], None, (w_o, [(first_a, 256), (first_a1, 128), (first_b, 256)])
        )
        v_xo = over_x(v_o)
        wa0, wa1, wb = over_y(rows_a0), over_y(rows_a1), over_y(rows_b)
        k_soa, k_sob, v_so = over_core(after(k_oa, v_o)), over_core(after(k_ob, v_o)), over_core(v_o)

        all_w, all_f = [w_k, w_v, w_q], [False, True, False]
        k_r0, v_r0, q_r0 = proj(after(x_f0, rows_b), all_w, all_f)
        k_xr0, v_xr0 = over_x(k_r0), over_x(v_r0)
        k_sr0, v_sr0 = over_core(k_r0), over_core(v_r0)
        own, own_s = ([(k_oa, k_ob)], [v_o]), ([(k_soa, k_sob)], [v_so])
        state_o = attend([after(q_o, q_r0)], [own, own_s], None, False, 4)

        k_r1, v_r1 = proj(after(x_f1, state_o[0]), [w_k, w_v], [False, True])
        k_xr1, v_xr1 = over_x(k_r1), over_x(v_r1)
        k_sr1, v_sr1 = over_core(k_r1), over_core(v_r1)
        v_sxo = over_core(after(v_xo, v_r1))
        (q_r1,) = proj(after(x_f1, v_r1), [w_q], [False])
        k_sxoa, k_sxob = over_core(after(k_xoa, q_r0)), over_core(after(k_xob, q_r0))
        far, far_s = ([k_r0, k_r1], [v_r0, v_r1]), ([k_sr0, k_sr1], [v_sr0, v_sr1])
        xo, xo_s = ([(k_xoa, k_xob)], [v_xo]), ([(k_sxoa, k_sxob)], [v_sxo])
        state_r = attend([q_r0, q_r1], [own, own_s, far, far_s, xo, xo_s], None, False, 2)
        k_sxr0, v_sxr0 = over_core(after(k_xr0, state_r[0])), over_core(after(v_xr0, state_r[0]))
        late = ([k_xr0, k_sxr0], [v_xr0, v_sxr0])
        state_o = attend([after(q_o, state_r[0])], [far, far_s, xo, xo_s], state_o, False, 1)
        wx0, wx1 = over_x(after(wa0, state_r[0])), over_x(after(wa1, state_o[0]))
        wa0_s, wa1_s = over_core(after(wa0, state_r[0])), over_core(after(wa1, state_o[0]))
        state_r = attend([after(q_r0, state_o[0]), q_r1], [late], state_r, False, 4)

        k_sxr1, v_sxr1 = over_core(after(k_xr1, state_r[0])), over_core(after(v_xr1, state_r[0]))
        latest = ([k_xr1, k_sxr1], [v_xr1, v_sxr1])
        o_ra = attend([after(q_r0, state_r[0]), q_r1], [latest], state_r, True, 4, chip)
        o_fa = over_y(o_ra)
        o_rb = attend([after(q_r0, o_ra), q_r1], [latest], state_r, True, 4, 1 - chip)
        o_fb = over_y(o_rb)
        wb_s = over_core(after(wb, o_rb))
        o_own = attend([after(q_o, o_rb)], [late, latest], state_o, True, 4)
        near = lambda core_of, more: lambda x, c: (x * 2 + core_of(c) * 3 + more) * 128
        away = lambda core_of, more: lambda x, c: ((1 - x) * 2 + core_of(c) * 3 + more) * 128
        same, other, zero = lambda c: c, lambda c: 1 - c, lambda x, c: 0
        pieces = [(w_o, 0, zero, None), (wa0, 1, near(same, 0), None), (wa0_s, 1, near(other, 0), None)]
        pieces += [(wa1, 1, near(same, 2), None), (wa1_s, 1, near(other, 2), None)]
        pieces.append(((wb, wb_s), 1, lambda x, c: (1 - x) * 768, lambda x, c: c == x))
        total = fold([o_own, o_fa], pieces, None, jnp.float32)
        wx0_s = over_core(after(wx0, total))
        wx1_s = over_core(after(wx1, total))
        pieces = [((wb, wb_s), 0, lambda x, c: x * 768, lambda x, c: c != x)]
        pieces += [(wx0, 0, away(same, 0), None), (wx0_s, 0, away(other, 0), None)]
        pieces += [(wx1, 0, away(same, 2), None), (wx1_s, 0, away(other, 2), None)]
        return fold([after(o_fb, wx1)], pieces, total, jnp.bfloat16)

    seq_spec = P(('dp', 'sp', 'hp'), None)
    in_specs = (seq_spec, P(None, 'hp'), P(None, 'hp'), P(None, 'hp'), P('hp', None))
    return jax.shard_map(device_fn, mesh=mesh, in_specs=in_specs, out_specs=seq_spec, check_vma=False)
```

```python
import functools
import math

import jax
import jax.numpy as jnp
from jax import lax
from jax.experimental import pallas as pl
from jax.experimental.pallas import tpu as pltpu
from jax.sharding import PartitionSpec as P


HEAD_DIM = 128
EXP2_SCALE = math.log2(math.e) / math.sqrt(HEAD_DIM)
CHUNK = 256
SUM_LIMIT = 2.0**60
ACC_LIMIT = 3.0e38


def attend_kernel(shape, heads, split, first, last, scalars, *refs):
    refs = list(refs)
    take = lambda n: [refs.pop(0) for _ in range(n)]
    take(scalars)
    q_refs = take(shape[0])
    groups = [([take(k) for k in widths], take(v)) for widths, v in shape[1:]]
    state_in = None if first else take(3)
    outs, q_copy = refs[:-1], refs[-1]
    low = pl.program_id(0) < split
    chunks = []
    for pieces, values in groups:
        k_parts = [(p, r) for p in pieces for r in range(0, p[0].shape[0], CHUNK)]
        v_parts = [(v, c) for v in values for c in range(0, v.shape[1], CHUNK)]
        chunks += [k + v for k, v in zip(k_parts, v_parts)]

    def scores_of(chunk, at, query):
        piece, row = chunk[:2]
        keys = piece[0][row:row + CHUNK, at]
        if len(piece) > 1:
            keys = jnp.where(low, keys, piece[1][row:row + CHUNK, at])
        return lax.dot_general(keys, query, (((1,), (1,)), ((), ())), preferred_element_type=jnp.float32)

    def values_of(chunk, at, probs):
        v, column = chunk[2:]
        return jnp.dot(v[at, column:column + CHUNK], probs, preferred_element_type=jnp.float32)

    fixed = [slice(h * HEAD_DIM, (h + 1) * HEAD_DIM) for h in range(heads)]
    queries = [jnp.concatenate([r[:, at] for r in q_refs], axis=0) for at in fixed]
    items = [(h, c) for c in range(len(chunks)) for h in range(heads)]
    depth = 2
    state = {} if first else {h: (state_in[0][h], state_in[1][h], state_in[2][fixed[h], :]) for h in range(heads)}
    score = lambda h, c: scores_of(chunks[c], fixed[h], queries[h])
    ahead = [score(*item) for item in items[:depth]]
    for i, (h, c) in enumerate(items):
        if i + depth < len(items):
            ahead.append(score(*items[i + depth]))
        scores = ahead.pop(0)
        shift = state[h][0] if h in state else jnp.max(scores, axis=0, keepdims=True) * EXP2_SCALE
        probs = jnp.exp2(scores * EXP2_SCALE - shift)
        part_sum = jnp.sum(probs, axis=0, keepdims=True)
        part = values_of(chunks[c], fixed[h], probs.astype(jnp.bfloat16))
        state[h] = (shift, state[h][1] + part_sum, state[h][2] + part) if h in state else (shift, part_sum, part)

    fine = None
    for h in range(heads):
        shift, run_sum, acc = state[h]
        good = jnp.logical_and(jnp.max(run_sum) < SUM_LIMIT, jnp.max(jnp.abs(acc)) < ACC_LIMIT)
        fine = good if fine is None else jnp.logical_and(fine, good)
        if last:
            outs[0][:, fixed[h]] = (acc / run_sum).T.astype(jnp.bfloat16)
        else:
            outs[0][h], outs[1][h], outs[2][fixed[h], :] = shift, run_sum, acc

    @pl.when(jnp.logical_not(fine))
    def _():
        row = 0
        for r in q_refs:
            q_copy[row:row + r.shape[0], :] = r[...]
            row += r.shape[0]

        def redo(n, carry):
            h = n // (row // HEAD_DIM)
            at = pl.ds(pl.multiple_of(h * HEAD_DIM, HEAD_DIM), HEAD_DIM)
            spot = pl.ds(pl.multiple_of((n % (row // HEAD_DIM)) * HEAD_DIM, HEAD_DIM), HEAD_DIM)
            query = q_copy[spot, at]
            if first:
                run_max = jnp.full((1, HEAD_DIM), -jnp.inf, jnp.float32)
                run_sum, acc = jnp.zeros((1, HEAD_DIM), jnp.float32), jnp.zeros((HEAD_DIM, HEAD_DIM), jnp.float32)
            else:
                run_max, run_sum, acc = state_in[0][h, :, spot], state_in[1][h, :, spot], state_in[2][at, spot]
            for chunk in chunks:
                scaled = scores_of(chunk, at, query) * EXP2_SCALE
                new_max = jnp.maximum(run_max, jnp.max(scaled, axis=0, keepdims=True))
                fade = jnp.exp2(run_max - new_max)
                probs = jnp.exp2(scaled - new_max)
                run_sum = run_sum * fade + jnp.sum(probs, axis=0, keepdims=True)
                acc = acc * fade + values_of(chunk, at, probs.astype(jnp.bfloat16))
                run_max = new_max
            if last:
                outs[0][spot, at] = (acc / run_sum).T.astype(jnp.bfloat16)
            else:
                outs[0][h, :, spot], outs[1][h, :, spot], outs[2][at, spot] = run_max, run_sum, acc
            return carry

        lax.fori_loop(0, heads * (row // HEAD_DIM), redo, 0)


def attend(queries, groups, state, last, block=1, part=None):
    rows, all_heads = sum(q.shape[0] for q in queries), queries[0].shape[1] // HEAD_DIM
    heads = all_heads if part is None else all_heads // 2
    width, steps = block * HEAD_DIM, heads // block
    split, offset = 0, () if part is None else (jnp.full((1,), part * steps, jnp.int32),)
    shift = lambda h, o: h + o[0][0] if o else h
    spec = lambda block, index: pl.BlockSpec(block, lambda h, *o: index(h, shift(h, o)))
    first = state is None
    state_specs = [
        spec((block, 1, rows), lambda h, g: (g, 0, 0)),
        spec((block, 1, rows), lambda h, g: (g, 0, 0)),
        spec((width, rows), lambda h, g: (g, 0)),
    ]
    state_shapes = [jax.ShapeDtypeStruct((all_heads, 1, rows), jnp.float32)] * 2
    state_shapes.append(jax.ShapeDtypeStruct((all_heads * HEAD_DIM, rows), jnp.float32))
    tall = lambda a: spec((a.shape[0], width), lambda h, g: (0, g))
    wide = lambda a: spec((width, a.shape[1]), lambda h, g: (g, 0))
    operands, in_specs, shape, key_rows = list(queries), [tall(q) for q in queries], [len(queries)], 0
    for keys, values_t in groups:
        widths = []
        for k in keys:
            if not isinstance(k, tuple):
                operands.append(k)
                in_specs.append(tall(k))
                widths.append(1)
            else:
                split = k[0].shape[1] // width
                operands += k
                in_specs.append(spec((k[0].shape[0], width), lambda h, g, s=split: (0, jnp.minimum(h, s - 1))))
                in_specs.append(spec((k[1].shape[0], width), lambda h, g, s=split: (0, jnp.maximum(h - s, 0))))
                widths.append(2)
        operands += values_t
        in_specs += [wide(v) for v in values_t]
        shape.append((tuple(widths), len(values_t)))
        key_rows += sum(v.shape[1] for v in values_t)
    count = len(operands)
    o_shape = jax.ShapeDtypeStruct((rows, heads * HEAD_DIM), jnp.bfloat16)
    return pl.pallas_call(
        functools.partial(attend_kernel, tuple(shape), block, split, first, last, len(offset)),
        grid_spec=pltpu.PrefetchScalarGridSpec(
            num_scalar_prefetch=len(offset),
            grid=(steps,),
            in_specs=in_specs + ([] if first else state_specs),
            out_specs=spec((rows, width), lambda h, g: (0, h)) if last else state_specs,
            scratch_shapes=[pltpu.VMEM((rows, width), jnp.bfloat16)],
        ),
        out_shape=o_shape if last else state_shapes,
        input_output_aliases={} if first or last else {len(offset) + count + j: j for j in range(3)},
        cost_estimate=pl.CostEstimate(
            flops=8 * rows * key_rows * heads * HEAD_DIM,
            bytes_accessed=2 * heads * HEAD_DIM * (rows + 2 * key_rows),
            transcendentals=rows * key_rows * heads,
        ),
        compiler_params=pltpu.CompilerParams(vmem_limit_bytes=62 * 2**20),
    )(*offset, *operands, *(state or ()))


def project_kernel(flips, width, ranges, rows_of, x_hbm, *refs):
    refs = list(refs)
    take = lambda n: [refs.pop(0) for _ in range(n)]
    count = len(flips)
    w_refs = take(count)
    source = take(1)[0] if rows_of and rows_of[0] is not None else None
    picks = rows_of[1] if rows_of else []
    o_refs, pick_refs = take(count), take(len(picks))
    x_ref, x_sem, ring, sems = take(4)
    stage = take(1)[0] if source is not None else None
    pick_sem = take(1)[0] if picks else None
    steps = [(stop - start) // width for start, stop in ranges]
    firsts = [sum(steps[:i]) for i in range(count)]

    def copy(i, step, slot):
        columns = pl.ds(pl.multiple_of(ranges[i][0] + step * width, width), width)
        return pltpu.make_async_copy(w_refs[i].at[:, columns], ring.at[slot], sems.at[slot])

    def fetch(n):
        for i in range(count):
            @pl.when(jnp.logical_and(n >= firsts[i], n < firsts[i] + steps[i]))
            def _():
                copy(i, n - firsts[i], lax.rem(n, 3)).start()

    def pick_copies(inward):
        copies, row = [], 0
        for j, (start, rows) in enumerate(picks):
            if source is None:
                copies.append(pltpu.make_async_copy(x_ref.at[pl.ds(start, rows)], pick_refs[j], pick_sem.at[j]))
                continue
            here = stage.at[pl.ds(row, rows)]
            row += rows
            if inward:
                there = source.at[pl.ds(pl.multiple_of(start(), 128), rows)]
                copies.append(pltpu.make_async_copy(there, here, pick_sem.at[j]))
            else:
                copies.append(pltpu.make_async_copy(here, pick_refs[j], pick_sem.at[j]))
        return copies

    x_copy = pltpu.make_async_copy(x_hbm, x_ref, x_sem)
    x_copy.start()
    fetch(jnp.int32(0))
    fetch(jnp.int32(1))
    x_copy.wait()
    for c in pick_copies(True):
        c.start()
    for i in range(count):
        def step(j, carry, i=i):
            n = firsts[i] + j
            slot = lax.rem(n, 3)
            fetch(n + 2)
            copy(i, j, slot).wait()
            block = jnp.dot(x_ref[...], ring[slot], preferred_element_type=jnp.float32)
            columns = pl.ds(pl.multiple_of(j * width, width), width)
            if flips[i]:
                o_refs[i][columns, :] = block.T.astype(jnp.bfloat16)
            else:
                o_refs[i][:, columns] = block.astype(jnp.bfloat16)
            return carry

        lax.fori_loop(0, steps[i], step, 0)
        if source is not None and i == 0:
            for inward, outward in zip(pick_copies(True), pick_copies(False)):
                inward.wait()
                outward.start()
    for c in pick_copies(False):
        c.wait()


def project(x, weights, flips, ranges=None, rows_of=None, width=512):
    rows, depth = x.shape
    ranges = ranges or [(0, w.shape[1]) for w in weights]
    counts = [stop - start for start, stop in ranges]
    shapes = [(c, rows) if f else (rows, c) for c, f in zip(counts, flips)]
    source, picks = rows_of or (None, [])
    any_spec, vmem_spec = pl.BlockSpec(memory_space=pl.ANY), pl.BlockSpec(memory_space=pltpu.VMEM)
    shapes += [(n, (x if source is None else source).shape[1]) for _, n in picks]
    scratch = [pltpu.VMEM(x.shape, jnp.bfloat16), pltpu.SemaphoreType.DMA(())]
    scratch += [pltpu.VMEM((3, depth, width), jnp.bfloat16), pltpu.SemaphoreType.DMA((3,))]
    if source is not None:
        scratch.append(pltpu.VMEM((sum(n for _, n in picks), source.shape[1]), jnp.bfloat16))
    if picks:
        scratch.append(pltpu.SemaphoreType.DMA((len(picks),)))
    static = None if not picks else ('source' if source is not None else None, tuple(picks))
    return pl.pallas_call(
        functools.partial(project_kernel, tuple(flips), width, tuple(ranges), static),
        in_specs=[any_spec] * (1 + len(weights) + (source is not None)),
        out_specs=[vmem_spec] * len(weights) + [any_spec] * len(picks),
        out_shape=[jax.ShapeDtypeStruct(s, jnp.bfloat16) for s in shapes],
        scratch_shapes=scratch,
        cost_estimate=pl.CostEstimate(
            flops=2 * rows * depth * sum(counts),
            bytes_accessed=2 * depth * sum(counts),
            transcendentals=0,
        ),
        compiler_params=pltpu.CompilerParams(vmem_limit_bytes=62 * 2**20),
    )(x, *weights, *(() if source is None else (source,)))


def fold_kernel(plan, width, has_base, *refs):
    refs = list(refs)
    take = lambda n: [refs.pop(0) for _ in range(n)]
    chip, core = lax.axis_index('sp') // 2, lax.axis_index('sp') % 2
    lhs_refs = take(max(p[1] for p in plan) + 1)
    piece_refs = [take(1 if p[3] is None else 2) for p in plan]
    base_ref = take(1)[0] if has_base else None
    out_ref, left, left_sem, right, right_sem, outs, out_sem = take(7)
    bases, base_sem = take(2) if has_base else (None, None)
    steps = out_ref.shape[1] // width
    columns = lambda j: pl.ds(pl.multiple_of(j * width, width), width)

    def fetches(j, slot):
        copies, row = [], 0
        for i, (depth, _, _, choice) in enumerate(plan):
            here = right.at[slot, pl.ds(row, depth)]
            versions = [pltpu.make_async_copy(r.at[:, columns(j)], here, right_sem.at[slot, i]) for r in piece_refs[i]]
            copies.append((versions, choice))
            row += depth
        if has_base:
            versions = [pltpu.make_async_copy(base_ref.at[:, columns(j)], bases.at[slot], base_sem.at[slot])]
            copies.append((versions, None))
        return copies

    def fetch(j):
        for versions, choice in fetches(j, lax.rem(j, 3)):
            if choice is None:
                versions[0].start()
                continue
            pl.when(choice(chip, core))(versions[0].start)
            pl.when(jnp.logical_not(choice(chip, core)))(versions[1].start)

    def store(j):
        slot = lax.rem(j, 2)
        return pltpu.make_async_copy(outs.at[slot], out_ref.at[:, columns(j)], out_sem.at[slot])

    lhs_copies, column = [], 0
    for i, (depth, which, start, _) in enumerate(plan):
        picked = pl.ds(pl.multiple_of(start(chip, core), 128), depth)
        source, here = lhs_refs[which].at[:, picked], left.at[:, column:column + depth]
        lhs_copies.append(pltpu.make_async_copy(source, here, left_sem.at[i]))
        lhs_copies[-1].start()
        column += depth
    fetch(jnp.int32(0))
    fetch(jnp.int32(1))
    for c in lhs_copies:
        c.wait()

    def step(j, carry):
        slot = lax.rem(j, 3)

        @pl.when(j + 2 < steps)
        def _():
            fetch(j + 2)

        for versions, _ in fetches(j, slot):
            versions[0].wait()

        total = jnp.dot(left[...], right[slot], preferred_element_type=jnp.float32)
        if has_base:
            total += bases[slot]

        @pl.when(j >= 2)
        def _():
            store(j - 2).wait()

        outs[lax.rem(j, 2)] = total.astype(out_ref.dtype)
        store(j).start()
        return carry

    lax.fori_loop(0, steps, step, 0)
    store(jnp.int32(steps - 2)).wait()
    store(jnp.int32(steps - 1)).wait()


def fold(lhs, pieces, base, dtype, width=512):
    plan, arrays = [], []
    for piece, which, start, choice in pieces:
        versions = piece if isinstance(piece, tuple) else (piece,)
        plan.append((versions[0].shape[0], which, start, choice))
        arrays += versions
    rows, columns, depth = lhs[0].shape[0], arrays[0].shape[1], sum(p[0] for p in plan)
    any_spec = pl.BlockSpec(memory_space=pl.ANY)
    scratch = [
        pltpu.VMEM((rows, depth), jnp.bfloat16),
        pltpu.SemaphoreType.DMA((len(plan),)),
        pltpu.VMEM((3, depth, width), jnp.bfloat16),
        pltpu.SemaphoreType.DMA((3, len(plan))),
        pltpu.VMEM((2, rows, width), dtype),
        pltpu.SemaphoreType.DMA((2,)),
    ]
    if base is not None:
        scratch += [pltpu.VMEM((3, rows, width), jnp.float32), pltpu.SemaphoreType.DMA((3,))]
    return pl.pallas_call(
        functools.partial(fold_kernel, tuple(plan), width, base is not None),
        in_specs=[any_spec] * (len(lhs) + len(arrays) + (base is not None)),
        out_specs=any_spec,
        out_shape=jax.ShapeDtypeStruct((rows, columns), dtype),
        scratch_shapes=scratch,
        cost_estimate=pl.CostEstimate(flops=2 * rows * columns * depth, bytes_accessed=2 * columns * depth, transcendentals=0),
        compiler_params=pltpu.CompilerParams(vmem_limit_bytes=62 * 2**20),
    )(*lhs, *arrays, *(() if base is None else (base,)))


def after(value, *tokens):
    return lax.optimization_barrier((value, *tokens))[0]


def solution(mesh):
    hp_swap = [(0, 1), (1, 0)]
    x_swap = [(0, 2), (1, 3), (2, 0), (3, 1)]
    core_swap = [(0, 1), (1, 0), (2, 3), (3, 2)]

    def device_fn(x_own, w_q, w_k, w_v, w_o):
        sp = lax.axis_index('sp')
        chip = sp // 2
        half = x_own.shape[0] // 2
        over_y = lambda a: lax.ppermute(a, 'hp', hp_swap)
        over_x = lambda a: lax.ppermute(a, 'sp', x_swap)
        over_core = lambda a: lax.ppermute(a, 'sp', core_swap)

        def proj(x, weights, flips, ranges=None, rows_of=None, width=512):
            return project(x, weights, flips, ranges, rows_of, width)

        unit_a = lambda chip_, core_: chip_ * 10 + core_ * 3
        unit_b = lambda core_: 6 + core_ * 2

        middle = w_k.shape[1] // 2
        k_oa, x_half0 = proj(x_own, [w_k], [False], [(0, middle)], (None, [(0, half)]), 256)
        k_xoa = over_x(k_oa)
        x_f0 = over_y(x_half0)
        k_ob, x_half = proj(after(x_own, k_oa), [w_k], [False], [(middle, 2 * middle)], (None, [(half, half)]))
        k_xob = over_x(k_ob)
        x_f1 = over_y(x_half)
        first_a = lambda: unit_a(lax.axis_index('sp') // 2, lax.axis_index('sp') % 2) * 128
        first_a1 = lambda: first_a() + 256
        first_b = lambda: unit_b(lax.axis_index('sp') % 2) * 128
        v_o, q_o, rows_a0, rows_a1, rows_b = proj(
            after(x_own, k_ob), [w_v, w_q], [True, False], None, (w_o, [(first_a, 256), (first_a1, 128), (first_b, 256)])
        )
        v_xo = over_x(v_o)
        wa0, wa1, wb = over_y(rows_a0), over_y(rows_a1), over_y(rows_b)
        k_soa, k_sob, v_so = over_core(after(k_oa, v_o)), over_core(after(k_ob, v_o)), over_core(v_o)

        all_w, all_f = [w_k, w_v, w_q], [False, True, False]
        k_r0, v_r0, q_r0 = proj(after(x_f0, rows_b), all_w, all_f)
        k_xr0, v_xr0 = over_x(k_r0), over_x(v_r0)
        k_sr0, v_sr0 = over_core(k_r0), over_core(v_r0)
        own, own_s = ([(k_oa, k_ob)], [v_o]), ([(k_soa, k_sob)], [v_so])
        state_o = attend([after(q_o, q_r0)], [own, own_s], None, False, 4)

        k_r1, v_r1 = proj(after(x_f1, state_o[0]), [w_k, w_v], [False, True])
        k_xr1, v_xr1 = over_x(k_r1), over_x(v_r1)
        k_sr1, v_sr1 = over_core(k_r1), over_core(v_r1)
        v_sxo = over_core(after(v_xo, v_r1))
        (q_r1,) = proj(after(x_f1, v_r1), [w_q], [False])
        k_sxoa, k_sxob = over_core(after(k_xoa, q_r0)), over_core(after(k_xob, q_r0))
        far, far_s = ([k_r0, k_r1], [v_r0, v_r1]), ([k_sr0, k_sr1], [v_sr0, v_sr1])
        xo, xo_s = ([(k_xoa, k_xob)], [v_xo]), ([(k_sxoa, k_sxob)], [v_sxo])
        state_r = attend([q_r0, q_r1], [own, own_s, far, far_s, xo, xo_s], None, False, 2)
        k_sxr0, v_sxr0 = over_core(after(k_xr0, state_r[0])), over_core(after(v_xr0, state_r[0]))
        late = ([k_xr0, k_sxr0], [v_xr0, v_sxr0])
        state_o = attend([after(q_o, state_r[0])], [far, far_s, xo, xo_s], state_o, False, 1)
        wx0, wx1 = over_x(after(wa0, state_r[0])), over_x(after(wa1, state_o[0]))
        wa0_s, wa1_s = over_core(after(wa0, state_r[0])), over_core(after(wa1, state_o[0]))
        state_r = attend([after(q_r0, state_o[0]), q_r1], [late], state_r, False, 4)

        k_sxr1, v_sxr1 = over_core(after(k_xr1, state_r[0])), over_core(after(v_xr1, state_r[0]))
        latest = ([k_xr1, k_sxr1], [v_xr1, v_sxr1])
        o_ra = attend([after(q_r0, state_r[0]), q_r1], [latest], state_r, True, 4, chip)
        o_fa = over_y(o_ra)
        o_rb = attend([after(q_r0, o_ra), q_r1], [latest], state_r, True, 4, 1 - chip)
        o_fb = over_y(o_rb)
        wb_s = over_core(after(wb, o_rb))
        o_own = attend([after(q_o, o_rb)], [late, latest], state_o, True, 4)
        near = lambda core_of, more: lambda x, c: (x * 2 + core_of(c) * 3 + more) * 128
        away = lambda core_of, more: lambda x, c: ((1 - x) * 2 + core_of(c) * 3 + more) * 128
        same, other, zero = lambda c: c, lambda c: 1 - c, lambda x, c: 0
        pieces = [(w_o, 0, zero, None), (wa0, 1, near(same, 0), None), (wa0_s, 1, near(other, 0), None)]
        pieces += [(wa1, 1, near(same, 2), None), (wa1_s, 1, near(other, 2), None)]
        pieces.append(((wb, wb_s), 1, lambda x, c: (1 - x) * 768, lambda x, c: c == x))
        total = fold([o_own, o_fa], pieces, None, jnp.float32)
        wx0_s = over_core(after(wx0, total))
        wx1_s = over_core(after(wx1, total))
        pieces = [((wb, wb_s), 0, lambda x, c: x * 768, lambda x, c: c != x)]
        pieces += [(wx0, 0, away(same, 0), None), (wx0_s, 0, away(other, 0), None)]
        pieces += [(wx1, 0, away(same, 2), None), (wx1_s, 0, away(other, 2), None)]
        return fold([after(o_fb, wx1)], pieces, total, jnp.bfloat16)

    seq_spec = P(('dp', 'sp', 'hp'), None)
    in_specs = (seq_spec, P(None, 'hp'), P(None, 'hp'), P(None, 'hp'), P('hp', None))
    return jax.shard_map(device_fn, mesh=mesh, in_specs=in_specs, out_specs=seq_spec, check_vma=False)
```

```python
import functools
import math

import jax
import jax.numpy as jnp
from jax import lax
from jax.experimental import pallas as pl
from jax.experimental.pallas import tpu as pltpu
from jax.sharding import PartitionSpec as P


HEAD_DIM = 128
EXP2_SCALE = math.log2(math.e) / math.sqrt(HEAD_DIM)
CHUNK = 256
SUM_LIMIT = 2.0**60
ACC_LIMIT = 3.0e38


def attend_kernel(shape, heads, split, first, last, scalars, *refs):
    refs = list(refs)
    take = lambda n: [refs.pop(0) for _ in range(n)]
    take(scalars)
    q_refs = take(shape[0])
    groups = [([take(k) for k in widths], take(v)) for widths, v in shape[1:]]
    state_in = None if first else take(3)
    outs, q_copy = refs[:-1], refs[-1]
    low = pl.program_id(0) < split
    chunks = []
    for pieces, values in groups:
        k_parts = [(p, r) for p in pieces for r in range(0, p[0].shape[0], CHUNK)]
        v_parts = [(v, c) for v in values for c in range(0, v.shape[1], CHUNK)]
        chunks += [k + v for k, v in zip(k_parts, v_parts)]

    def scores_of(chunk, at, query):
        piece, row = chunk[:2]
        keys = piece[0][row:row + CHUNK, at]
        if len(piece) > 1:
            keys = jnp.where(low, keys, piece[1][row:row + CHUNK, at])
        return lax.dot_general(keys, query, (((1,), (1,)), ((), ())), preferred_element_type=jnp.float32)

    def values_of(chunk, at, probs):
        v, column = chunk[2:]
        return jnp.dot(v[at, column:column + CHUNK], probs, preferred_element_type=jnp.float32)

    fixed = [slice(h * HEAD_DIM, (h + 1) * HEAD_DIM) for h in range(heads)]
    queries = [jnp.concatenate([r[:, at] for r in q_refs], axis=0) for at in fixed]
    items = [(h, c) for c in range(len(chunks)) for h in range(heads)]
    depth = 2
    state = {} if first else {h: (state_in[0][h], state_in[1][h], state_in[2][fixed[h], :]) for h in range(heads)}
    score = lambda h, c: scores_of(chunks[c], fixed[h], queries[h])
    ahead = [score(*item) for item in items[:depth]]
    for i, (h, c) in enumerate(items):
        if i + depth < len(items):
            ahead.append(score(*items[i + depth]))
        scores = ahead.pop(0)
        shift = state[h][0] if h in state else jnp.max(scores, axis=0, keepdims=True) * EXP2_SCALE
        probs = jnp.exp2(scores * EXP2_SCALE - shift)
        part_sum = jnp.sum(probs, axis=0, keepdims=True)
        part = values_of(chunks[c], fixed[h], probs.astype(jnp.bfloat16))
        state[h] = (shift, state[h][1] + part_sum, state[h][2] + part) if h in state else (shift, part_sum, part)

    fine = None
    for h in range(heads):
        shift, run_sum, acc = state[h]
        good = jnp.logical_and(jnp.max(run_sum) < SUM_LIMIT, jnp.max(jnp.abs(acc)) < ACC_LIMIT)
        fine = good if fine is None else jnp.logical_and(fine, good)
        if last:
            outs[0][:, fixed[h]] = (acc / run_sum).T.astype(jnp.bfloat16)
        else:
            outs[0][h], outs[1][h], outs[2][fixed[h], :] = shift, run_sum, acc

    @pl.when(jnp.logical_not(fine))
    def _():
        row = 0
        for r in q_refs:
            q_copy[row:row + r.shape[0], :] = r[...]
            row += r.shape[0]

        def redo(n, carry):
            h = n // (row // HEAD_DIM)
            at = pl.ds(pl.multiple_of(h * HEAD_DIM, HEAD_DIM), HEAD_DIM)
            spot = pl.ds(pl.multiple_of((n % (row // HEAD_DIM)) * HEAD_DIM, HEAD_DIM), HEAD_DIM)
            query = q_copy[spot, at]
            if first:
                run_max = jnp.full((1, HEAD_DIM), -jnp.inf, jnp.float32)
                run_sum, acc = jnp.zeros((1, HEAD_DIM), jnp.float32), jnp.zeros((HEAD_DIM, HEAD_DIM), jnp.float32)
            else:
                run_max, run_sum, acc = state_in[0][h, :, spot], state_in[1][h, :, spot], state_in[2][at, spot]
            for chunk in chunks:
                scaled = scores_of(chunk, at, query) * EXP2_SCALE
                new_max = jnp.maximum(run_max, jnp.max(scaled, axis=0, keepdims=True))
                fade = jnp.exp2(run_max - new_max)
                probs = jnp.exp2(scaled - new_max)
                run_sum = run_sum * fade + jnp.sum(probs, axis=0, keepdims=True)
                acc = acc * fade + values_of(chunk, at, probs.astype(jnp.bfloat16))
                run_max = new_max
            if last:
                outs[0][spot, at] = (acc / run_sum).T.astype(jnp.bfloat16)
            else:
                outs[0][h, :, spot], outs[1][h, :, spot], outs[2][at, spot] = run_max, run_sum, acc
            return carry

        lax.fori_loop(0, heads * (row // HEAD_DIM), redo, 0)


def attend(queries, groups, state, last, block=1, part=None):
    rows, all_heads = sum(q.shape[0] for q in queries), queries[0].shape[1] // HEAD_DIM
    heads = all_heads if part is None else all_heads // 2
    width, steps = block * HEAD_DIM, heads // block
    split, offset = 0, () if part is None else (jnp.full((1,), part * steps, jnp.int32),)
    shift = lambda h, o: h + o[0][0] if o else h
    spec = lambda block, index: pl.BlockSpec(block, lambda h, *o: index(h, shift(h, o)))
    first = state is None
    state_specs = [
        spec((block, 1, rows), lambda h, g: (g, 0, 0)),
        spec((block, 1, rows), lambda h, g: (g, 0, 0)),
        spec((width, rows), lambda h, g: (g, 0)),
    ]
    state_shapes = [jax.ShapeDtypeStruct((all_heads, 1, rows), jnp.float32)] * 2
    state_shapes.append(jax.ShapeDtypeStruct((all_heads * HEAD_DIM, rows), jnp.float32))
    tall = lambda a: spec((a.shape[0], width), lambda h, g: (0, g))
    wide = lambda a: spec((width, a.shape[1]), lambda h, g: (g, 0))
    operands, in_specs, shape, key_rows = list(queries), [tall(q) for q in queries], [len(queries)], 0
    for keys, values_t in groups:
        widths = []
        for k in keys:
            if not isinstance(k, tuple):
                operands.append(k)
                in_specs.append(tall(k))
                widths.append(1)
            else:
                split = k[0].shape[1] // width
                operands += k
                in_specs.append(spec((k[0].shape[0], width), lambda h, g, s=split: (0, jnp.minimum(h, s - 1))))
                in_specs.append(spec((k[1].shape[0], width), lambda h, g, s=split: (0, jnp.maximum(h - s, 0))))
                widths.append(2)
        operands += values_t
        in_specs += [wide(v) for v in values_t]
        shape.append((tuple(widths), len(values_t)))
        key_rows += sum(v.shape[1] for v in values_t)
    count = len(operands)
    o_shape = jax.ShapeDtypeStruct((rows, heads * HEAD_DIM), jnp.bfloat16)
    return pl.pallas_call(
        functools.partial(attend_kernel, tuple(shape), block, split, first, last, len(offset)),
        grid_spec=pltpu.PrefetchScalarGridSpec(
            num_scalar_prefetch=len(offset),
            grid=(steps,),
            in_specs=in_specs + ([] if first else state_specs),
            out_specs=spec((rows, width), lambda h, g: (0, h)) if last else state_specs,
            scratch_shapes=[pltpu.VMEM((rows, width), jnp.bfloat16)],
        ),
        out_shape=o_shape if last else state_shapes,
        input_output_aliases={} if first or last else {len(offset) + count + j: j for j in range(3)},
        cost_estimate=pl.CostEstimate(
            flops=8 * rows * key_rows * heads * HEAD_DIM,
            bytes_accessed=2 * heads * HEAD_DIM * (rows + 2 * key_rows),
            transcendentals=rows * key_rows * heads,
        ),
        compiler_params=pltpu.CompilerParams(vmem_limit_bytes=62 * 2**20),
    )(*offset, *operands, *(state or ()))


def project_kernel(flips, width, ranges, rows_of, x_hbm, *refs):
    refs = list(refs)
    take = lambda n: [refs.pop(0) for _ in range(n)]
    count = len(flips)
    w_refs = take(count)
    source = take(1)[0] if rows_of and rows_of[0] is not None else None
    picks = rows_of[1] if rows_of else []
    o_refs, pick_refs = take(count), take(len(picks))
    x_ref, x_sem, ring, sems = take(4)
    stage = take(1)[0] if source is not None else None
    pick_sem = take(1)[0] if picks else None
    steps = [(stop - start) // width for start, stop in ranges]
    firsts = [sum(steps[:i]) for i in range(count)]

    def copy(i, step, slot):
        columns = pl.ds(pl.multiple_of(ranges[i][0] + step * width, width), width)
        return pltpu.make_async_copy(w_refs[i].at[:, columns], ring.at[slot], sems.at[slot])

    def fetch(n):
        for i in range(count):
            @pl.when(jnp.logical_and(n >= firsts[i], n < firsts[i] + steps[i]))
            def _():
                copy(i, n - firsts[i], lax.rem(n, 3)).start()

    def pick_copies(inward):
        copies, row = [], 0
        for j, (start, rows) in enumerate(picks):
            if source is None:
                copies.append(pltpu.make_async_copy(x_ref.at[pl.ds(start, rows)], pick_refs[j], pick_sem.at[j]))
                continue
            here = stage.at[pl.ds(row, rows)]
            row += rows
            if inward:
                there = source.at[pl.ds(pl.multiple_of(start(), 128), rows)]
                copies.append(pltpu.make_async_copy(there, here, pick_sem.at[j]))
            else:
                copies.append(pltpu.make_async_copy(here, pick_refs[j], pick_sem.at[j]))
        return copies

    x_copy = pltpu.make_async_copy(x_hbm, x_ref, x_sem)
    x_copy.start()
    fetch(jnp.int32(0))
    fetch(jnp.int32(1))
    x_copy.wait()
    for c in pick_copies(True):
        c.start()
    for i in range(count):
        def step(j, carry, i=i):
            n = firsts[i] + j
            slot = lax.rem(n, 3)
            fetch(n + 2)
            copy(i, j, slot).wait()
            block = jnp.dot(x_ref[...], ring[slot], preferred_element_type=jnp.float32)
            columns = pl.ds(pl.multiple_of(j * width, width), width)
            if flips[i]:
                o_refs[i][columns, :] = block.T.astype(jnp.bfloat16)
            else:
                o_refs[i][:, columns] = block.astype(jnp.bfloat16)
            return carry

        lax.fori_loop(0, steps[i], step, 0)
        if source is not None and i == 0:
            for inward, outward in zip(pick_copies(True), pick_copies(False)):
                inward.wait()
                outward.start()
    for c in pick_copies(False):
        c.wait()


def project(x, weights, flips, ranges=None, rows_of=None, width=512):
    rows, depth = x.shape
    ranges = ranges or [(0, w.shape[1]) for w in weights]
    counts = [stop - start for start, stop in ranges]
    shapes = [(c, rows) if f else (rows, c) for c, f in zip(counts, flips)]
    source, picks = rows_of or (None, [])
    any_spec, vmem_spec = pl.BlockSpec(memory_space=pl.ANY), pl.BlockSpec(memory_space=pltpu.VMEM)
    shapes += [(n, (x if source is None else source).shape[1]) for _, n in picks]
    scratch = [pltpu.VMEM(x.shape, jnp.bfloat16), pltpu.SemaphoreType.DMA(())]
    scratch += [pltpu.VMEM((3, depth, width), jnp.bfloat16), pltpu.SemaphoreType.DMA((3,))]
    if source is not None:
        scratch.append(pltpu.VMEM((sum(n for _, n in picks), source.shape[1]), jnp.bfloat16))
    if picks:
        scratch.append(pltpu.SemaphoreType.DMA((len(picks),)))
    static = None if not picks else ('source' if source is not None else None, tuple(picks))
    return pl.pallas_call(
        functools.partial(project_kernel, tuple(flips), width, tuple(ranges), static),
        in_specs=[any_spec] * (1 + len(weights) + (source is not None)),
        out_specs=[vmem_spec] * len(weights) + [any_spec] * len(picks),
        out_shape=[jax.ShapeDtypeStruct(s, jnp.bfloat16) for s in shapes],
        scratch_shapes=scratch,
        cost_estimate=pl.CostEstimate(
            flops=2 * rows * depth * sum(counts),
            bytes_accessed=2 * depth * sum(counts),
            transcendentals=0,
        ),
        compiler_params=pltpu.CompilerParams(vmem_limit_bytes=62 * 2**20),
    )(x, *weights, *(() if source is None else (source,)))


def fold_kernel(plan, width, has_base, *refs):
    refs = list(refs)
    take = lambda n: [refs.pop(0) for _ in range(n)]
    chip, core = lax.axis_index('sp') // 2, lax.axis_index('sp') % 2
    lhs_refs = take(max(p[1] for p in plan) + 1)
    piece_refs = [take(1 if p[3] is None else 2) for p in plan]
    base_ref = take(1)[0] if has_base else None
    out_ref, left, left_sem, right, right_sem, outs, out_sem = take(7)
    bases, base_sem = take(2) if has_base else (None, None)
    steps = out_ref.shape[1] // width
    columns = lambda j: pl.ds(pl.multiple_of(j * width, width), width)

    def fetches(j, slot):
        copies, row = [], 0
        for i, (depth, _, _, choice) in enumerate(plan):
            here = right.at[slot, pl.ds(row, depth)]
            versions = [pltpu.make_async_copy(r.at[:, columns(j)], here, right_sem.at[slot, i]) for r in piece_refs[i]]
            copies.append((versions, choice))
            row += depth
        if has_base:
            versions = [pltpu.make_async_copy(base_ref.at[:, columns(j)], bases.at[slot], base_sem.at[slot])]
            copies.append((versions, None))
        return copies

    def fetch(j):
        for versions, choice in fetches(j, lax.rem(j, 3)):
            if choice is None:
                versions[0].start()
                continue
            pl.when(choice(chip, core))(versions[0].start)
            pl.when(jnp.logical_not(choice(chip, core)))(versions[1].start)

    def store(j):
        slot = lax.rem(j, 2)
        return pltpu.make_async_copy(outs.at[slot], out_ref.at[:, columns(j)], out_sem.at[slot])

    lhs_copies, column = [], 0
    for i, (depth, which, start, _) in enumerate(plan):
        picked = pl.ds(pl.multiple_of(start(chip, core), 128), depth)
        source, here = lhs_refs[which].at[:, picked], left.at[:, column:column + depth]
        lhs_copies.append(pltpu.make_async_copy(source, here, left_sem.at[i]))
        lhs_copies[-1].start()
        column += depth
    fetch(jnp.int32(0))
    fetch(jnp.int32(1))
    for c in lhs_copies:
        c.wait()

    def step(j, carry):
        slot = lax.rem(j, 3)

        @pl.when(j + 2 < steps)
        def _():
            fetch(j + 2)

        for versions, _ in fetches(j, slot):
            versions[0].wait()

        total = jnp.dot(left[...], right[slot], preferred_element_type=jnp.float32)
        if has_base:
            total += bases[slot]

        @pl.when(j >= 2)
        def _():
            store(j - 2).wait()

        outs[lax.rem(j, 2)] = total.astype(out_ref.dtype)
        store(j).start()
        return carry

    lax.fori_loop(0, steps, step, 0)
    store(jnp.int32(steps - 2)).wait()
    store(jnp.int32(steps - 1)).wait()


def fold(lhs, pieces, base, dtype, width=512):
    plan, arrays = [], []
    for piece, which, start, choice in pieces:
        versions = piece if isinstance(piece, tuple) else (piece,)
        plan.append((versions[0].shape[0], which, start, choice))
        arrays += versions
    rows, columns, depth = lhs[0].shape[0], arrays[0].shape[1], sum(p[0] for p in plan)
    any_spec = pl.BlockSpec(memory_space=pl.ANY)
    scratch = [
        pltpu.VMEM((rows, depth), jnp.bfloat16),
        pltpu.SemaphoreType.DMA((len(plan),)),
        pltpu.VMEM((3, depth, width), jnp.bfloat16),
        pltpu.SemaphoreType.DMA((3, len(plan))),
        pltpu.VMEM((2, rows, width), dtype),
        pltpu.SemaphoreType.DMA((2,)),
    ]
    if base is not None:
        scratch += [pltpu.VMEM((3, rows, width), jnp.float32), pltpu.SemaphoreType.DMA((3,))]
    return pl.pallas_call(
        functools.partial(fold_kernel, tuple(plan), width, base is not None),
        in_specs=[any_spec] * (len(lhs) + len(arrays) + (base is not None)),
        out_specs=any_spec,
        out_shape=jax.ShapeDtypeStruct((rows, columns), dtype),
        scratch_shapes=scratch,
        cost_estimate=pl.CostEstimate(flops=2 * rows * columns * depth, bytes_accessed=2 * columns * depth, transcendentals=0),
        compiler_params=pltpu.CompilerParams(vmem_limit_bytes=62 * 2**20),
    )(*lhs, *arrays, *(() if base is None else (base,)))


def after(value, *tokens):
    return lax.optimization_barrier((value, *tokens))[0]


def solution(mesh):
    hp_swap = [(0, 1), (1, 0)]
    x_swap = [(0, 2), (1, 3), (2, 0), (3, 1)]
    core_swap = [(0, 1), (1, 0), (2, 3), (3, 2)]

    def device_fn(x_own, w_q, w_k, w_v, w_o):
        sp = lax.axis_index('sp')
        chip = sp // 2
        half = x_own.shape[0] // 2
        over_y = lambda a: lax.ppermute(a, 'hp', hp_swap)
        over_x = lambda a: lax.ppermute(a, 'sp', x_swap)
        over_core = lambda a: lax.ppermute(a, 'sp', core_swap)

        def proj(x, weights, flips, ranges=None, rows_of=None, width=512):
            return project(x, weights, flips, ranges, rows_of, width)

        unit_a = lambda chip_, core_: chip_ * 10 + core_ * 3
        unit_b = lambda core_: 6 + core_ * 2

        middle = w_k.shape[1] * 3 // 8
        k_oa, x_half0 = proj(x_own, [w_k], [False], [(0, middle)], (None, [(0, half)]), 256)
        k_xoa = over_x(k_oa)
        x_f0 = over_y(x_half0)
        k_ob, x_half = proj(after(x_own, k_oa), [w_k], [False], [(middle, w_k.shape[1])], (None, [(half, half)]), 256)
        k_xob = over_x(k_ob)
        x_f1 = over_y(x_half)
        first_a = lambda: unit_a(lax.axis_index('sp') // 2, lax.axis_index('sp') % 2) * 128
        first_a1 = lambda: first_a() + 256
        first_b = lambda: unit_b(lax.axis_index('sp') % 2) * 128
        v_o, q_o, rows_a0, rows_a1, rows_b = proj(
            after(x_own, k_ob), [w_v, w_q], [True, False], None, (w_o, [(first_a, 256), (first_a1, 128), (first_b, 256)])
        )
        v_xo = over_x(v_o)
        wa0, wa1, wb = over_y(rows_a0), over_y(rows_a1), over_y(rows_b)
        k_soa, k_sob, v_so = over_core(after(k_oa, v_o)), over_core(after(k_ob, v_o)), over_core(v_o)

        all_w, all_f = [w_k, w_v, w_q], [False, True, False]
        k_r0, v_r0, q_r0 = proj(after(x_f0, rows_b), all_w, all_f)
        k_xr0, v_xr0 = over_x(k_r0), over_x(v_r0)
        k_sr0, v_sr0 = over_core(k_r0), over_core(v_r0)
        own, own_s = ([(k_oa, k_ob)], [v_o]), ([(k_soa, k_sob)], [v_so])
        state_o = attend([after(q_o, q_r0)], [own, own_s], None, False, 2)

        k_r1, v_r1 = proj(after(x_f1, state_o[0]), [w_k, w_v], [False, True])
        k_xr1, v_xr1 = over_x(k_r1), over_x(v_r1)
        k_sr1, v_sr1 = over_core(k_r1), over_core(v_r1)
        v_sxo = over_core(after(v_xo, v_r1))
        (q_r1,) = proj(after(x_f1, v_r1), [w_q], [False])
        k_sxoa, k_sxob = over_core(after(k_xoa, q_r0)), over_core(after(k_xob, q_r0))
        far, far_s = ([k_r0, k_r1], [v_r0, v_r1]), ([k_sr0, k_sr1], [v_sr0, v_sr1])
        xo, xo_s = ([(k_xoa, k_xob)], [v_xo]), ([(k_sxoa, k_sxob)], [v_sxo])
        state_r = attend([q_r0, q_r1], [own, own_s, far, far_s, xo, xo_s], None, False, 2)
        k_sxr0, v_sxr0 = over_core(after(k_xr0, state_r[0])), over_core(after(v_xr0, state_r[0]))
        late = ([k_xr0, k_sxr0], [v_xr0, v_sxr0])
        state_o = attend([after(q_o, state_r[0])], [far, far_s, xo, xo_s], state_o, False, 1)
        wx0, wx1 = over_x(after(wa0, state_r[0])), over_x(after(wa1, state_o[0]))
        wa0_s, wa1_s = over_core(after(wa0, state_r[0])), over_core(after(wa1, state_o[0]))
        state_r = attend([after(q_r0, state_o[0]), q_r1], [late], state_r, False, 4)

        k_sxr1, v_sxr1 = over_core(after(k_xr1, state_r[0])), over_core(after(v_xr1, state_r[0]))
        latest = ([k_xr1, k_sxr1], [v_xr1, v_sxr1])
        o_ra = attend([after(q_r0, state_r[0]), q_r1], [latest], state_r, True, 4, chip)
        o_fa = over_y(o_ra)
        o_rb = attend([after(q_r0, o_ra), q_r1], [latest], state_r, True, 4, 1 - chip)
        o_fb = over_y(o_rb)
        wb_s = over_core(after(wb, o_rb))
        o_own = attend([after(q_o, o_rb)], [late, latest], state_o, True, 4)
        near = lambda core_of, more: lambda x, c: (x * 2 + core_of(c) * 3 + more) * 128
        away = lambda core_of, more: lambda x, c: ((1 - x) * 2 + core_of(c) * 3 + more) * 128
        same, other, zero = lambda c: c, lambda c: 1 - c, lambda x, c: 0
        pieces = [(w_o, 0, zero, None), (wa0, 1, near(same, 0), None), (wa0_s, 1, near(other, 0), None)]
        pieces += [(wa1, 1, near(same, 2), None), (wa1_s, 1, near(other, 2), None)]
        pieces.append(((wb, wb_s), 1, lambda x, c: (1 - x) * 768, lambda x, c: c == x))
        total = fold([o_own, o_fa], pieces, None, jnp.float32)
        wx0_s = over_core(after(wx0, total))
        wx1_s = over_core(after(wx1, total))
        pieces = [((wb, wb_s), 0, lambda x, c: x * 768, lambda x, c: c != x)]
        pieces += [(wx0, 0, away(same, 0), None), (wx0_s, 0, away(other, 0), None)]
        pieces += [(wx1, 0, away(same, 2), None), (wx1_s, 0, away(other, 2), None)]
        return fold([after(o_fb, wx1)], pieces, total, jnp.bfloat16, 1024)

    seq_spec = P(('dp', 'sp', 'hp'), None)
    in_specs = (seq_spec, P(None, 'hp'), P(None, 'hp'), P(None, 'hp'), P('hp', None))
    return jax.shard_map(device_fn, mesh=mesh, in_specs=in_specs, out_specs=seq_spec, check_vma=False)
```
